256 devices in a mesh: slab: 128 (over z, y_lo, x, core), layer: 2 (over y_hi).
Axes of the slice: x: 4, y: 4 (y_hi: 2, y_lo: 2; y = y_hi * 2 + y_lo), z: 8, core: 2. Of those that a mesh axis runs over, the one named last changes fastest.
Arguments:
- nodal_field: float32 [2, 8192, 4, 4, 512], P('layer', 'slab'), may hold values from -6 to 6
- metric: float32 [2, 8192, 4, 4, 3, 512], P('layer', 'slab'), may hold values from 0.25 to 2
- slab_ids: int32 [8192], replicated, may hold values from 0 to 8191, as said below
- face_map: int32 [8192, 1024], P('slab'), may hold values from 0 to 1023, as said below
Outputs:
- assembled: float32 [2, 8192, 4, 4, 512], P('layer', 'slab')
The draws below stay inside these ranges and needn't reach their ends.
Inputs may be any that keep to these rules, and one draw needn't show every extreme that they name: slab_ids is a permutation of 0 to 8191; positions p of one device are those with p // 64 equal to its index along slab, and for one rotation R every device holds exactly the slabs g with (g + R) mod 128 equal to its index, in any order of its positions, so slab (g + 1) mod 8192 always sits on the next device along slab, cyclically. Each row of face_map is a permutation of 0 to 1023: either the identity, or the map that reverses y, sending (ez, ey, c, b) to (ez, 3 - ey, c, 7 - b); z order is never changed.
All inputs are finite; a program needn't handle non-finite values.
Results may differ from the reference program's by a relative error of at most 0.00005.
Values sent between devices are 32-bit elements; how exact they have to be, the bound alone decides.
A program may use at most 192 MiB of HBM per device.

```python
import math
import jax
import jax.numpy as jnp
import numpy as np
from jax import lax

P_SIZE = 8
PTS = 512
EY = 4
EZ = 4
SLAB_DEV = 64
FACE = 1024
SLABS = 8192
LAYERS = 2
N_SLAB = 128


def permute_slots(sub_key):
    return jax.random.permutation(sub_key, SLAB_DEV)


def draw_slab_ids(key, part):
    rotate_key = jax.random.fold_in(key, 11)
    order_key = jax.random.fold_in(key, 12)
    rotation = jax.random.randint(rotate_key, (), 0, N_SLAB)
    key_list = jax.random.split(order_key, N_SLAB)
    slot_orders = jax.vmap(permute_slots)(key_list).astype(jnp.int32)
    residues = (jnp.arange(N_SLAB, dtype=jnp.int32) - rotation + N_SLAB) % N_SLAB
    return (slot_orders * N_SLAB + residues[:, None]).reshape(SLABS).astype(jnp.int32)


def draw_face_map(key, part):
    flip_key = jax.random.fold_in(key, 21)
    flip_bits = jax.random.randint(flip_key, (SLABS, 1), 0, 2)
    point_index = jnp.arange(FACE, dtype=jnp.int32)
    column = point_index % P_SIZE
    element_col = point_index // (P_SIZE * P_SIZE) % EY
    reversed_index = point_index + (P_SIZE - 1 - 2 * column) + (EY - 1 - 2 * element_col) * P_SIZE * P_SIZE
    return jnp.where(flip_bits == 1, reversed_index[None, :], point_index[None, :]).astype(jnp.int32)


def steps_of(rng, dims, shards, low, high):
    loudness, own = 1.0, jax.random.fold_in(rng, 6)
    for position, parts in shards:
        steps = jnp.exp(jax.random.uniform(jax.random.fold_in(own, position), (parts,), jnp.float32, low / len(shards), high / len(shards)))
        loudness = loudness * jnp.repeat(steps, dims[position] // parts).reshape([-1 if axis == position else 1 for axis in range(len(dims))])
    return loudness


def noise(key, shape, spread, limit, cuts=(), kind=jnp.bfloat16):
    drawn = spread * jax.random.normal(key, shape, jnp.float32)
    if cuts:
        drawn = drawn * steps_of(key, shape, cuts, -0.22, 0.18)
    return jnp.clip(drawn, -limit, limit).astype(kind)


def setup_inputs(seed: int = 0) -> dict:
    arg_keys = jax.random.split(jax.random.key(seed), 5)
    nodal_field = noise(arg_keys[0], (LAYERS, SLABS, EZ, EY, PTS), 1.0, 6.0, ((0, 2), (1, 128)), jnp.float32)
    metric = jnp.clip(jnp.exp(math.log(2.0) - 2.0794415 * jax.random.uniform(arg_keys[1], (LAYERS, SLABS, EZ, EY, 3, PTS), jnp.float32) ** steps_of(arg_keys[1], (LAYERS, SLABS, EZ, EY, 3, PTS), ((0, 2), (1, 128)), -0.2, 0.2)), 0.25, 2.0)
    slab_ids = draw_slab_ids(jax.random.fold_in(arg_keys[4], 71), 0)
    face_map = draw_face_map(jax.random.fold_in(arg_keys[4], 71), 0)
    return dict(nodal_field=nodal_field, metric=metric, slab_ids=slab_ids, face_map=face_map)


def legendre_pair(gll_nodes, degree):
    lower_poly = gll_nodes * 0.0 + 1.0
    upper_poly = gll_nodes.copy()
    for poly_order in range(2, degree + 1):
        lower_poly, upper_poly = upper_poly, ((2 * poly_order - 1) * gll_nodes * upper_poly - (poly_order - 1) * lower_poly) / poly_order
    return lower_poly, upper_poly


def gll_tables():
    degree = P_SIZE - 1
    gll_nodes = -np.cos(np.pi * np.arange(P_SIZE) / degree)
    for newton_sweep in range(100):
        lower_poly, upper_poly = legendre_pair(gll_nodes, degree)
        gll_nodes = gll_nodes - (gll_nodes * upper_poly - lower_poly) / ((degree + 1) * upper_poly)
    lower_poly, upper_poly = legendre_pair(gll_nodes, degree)
    quad_weights = 2.0 / (degree * (degree + 1) * upper_poly * upper_poly)
    identity = np.eye(P_SIZE)
    differ = gll_nodes[:, None] - gll_nodes[None, :] + identity
    derivative = upper_poly[:, None] / (upper_poly[None, :] * differ)
    derivative = derivative * (1.0 - identity)
    derivative[0, 0] = -degree * (degree + 1) / 4.0
    derivative[degree, degree] = degree * (degree + 1) / 4.0
    weight_cube = quad_weights[:, None, None] * quad_weights[None, :, None] * quad_weights[None, None, :]
    return jnp.asarray(derivative, jnp.float32), jnp.asarray(weight_cube, jnp.float32)


def local_apply(values, factors, derivative, weight_cube):
    highest = lax.Precision.HIGHEST
    grad_x = jnp.einsum("ai,...cbi->...cba", derivative, values, precision=highest)
    grad_y = jnp.einsum("bi,...cia->...cba", derivative, values, precision=highest)
    grad_z = jnp.einsum("ci,...iba->...cba", derivative, values, precision=highest)
    flux_x = weight_cube * factors[..., 0, :, :, :] * grad_x
    flux_y = weight_cube * factors[..., 1, :, :, :] * grad_y
    flux_z = weight_cube * factors[..., 2, :, :, :] * grad_z
    result = jnp.einsum("ia,...cbi->...cba", derivative, flux_x, precision=highest)
    result = result + jnp.einsum("ib,...cia->...cba", derivative, flux_y, precision=highest)
    result = result + jnp.einsum("ic,...iba->...cba", derivative, flux_z, precision=highest)
    return result


def assemble_slab(values):
    shared = values[..., :, :-1, :, P_SIZE - 1, :] + values[..., :, 1:, :, 0, :]
    values = values.at[..., :, :-1, :, P_SIZE - 1, :].set(shared)
    values = values.at[..., :, 1:, :, 0, :].set(shared)
    shared = values[..., :-1, :, P_SIZE - 1, :, :] + values[..., 1:, :, 0, :, :]
    values = values.at[..., :-1, :, P_SIZE - 1, :, :].set(shared)
    values = values.at[..., 1:, :, 0, :, :].set(shared)
    return values


def face_of(local_out, column):
    return local_out[..., column].reshape(local_out.shape[:-5] + (FACE,))


def put_face(local_out, face_values, column):
    return local_out.at[..., column].set(face_values.reshape(local_out.shape[:-1]))


def reference(nodal_field, metric, slab_ids, face_map):
    derivative, weight_cube = gll_tables()
    values = nodal_field.reshape(LAYERS * N_SLAB, SLAB_DEV, EZ, EY, P_SIZE, P_SIZE, P_SIZE)
    factors = metric.reshape(LAYERS * N_SLAB, SLAB_DEV, EZ, EY, 3, P_SIZE, P_SIZE, P_SIZE)

    def slab_block(pair_in):
        return assemble_slab(local_apply(pair_in[0], pair_in[1], derivative, weight_cube))

    local_out = lax.map(slab_block, (values, factors)).reshape(LAYERS, SLABS, EZ, EY, P_SIZE, P_SIZE, P_SIZE)
    slab_iota = jnp.arange(SLABS, dtype=jnp.int32)
    inverse = jnp.zeros((SLABS,), jnp.int32).at[slab_ids].set(slab_iota)
    next_pos = inverse[(slab_ids + 1) % SLABS]
    prev_pos = inverse[(slab_ids + SLABS - 1) % SLABS]
    right_face = face_of(local_out, P_SIZE - 1)
    left_face = face_of(local_out, 0)
    reoriented = jnp.zeros_like(right_face).at[:, slab_iota[:, None], face_map].set(right_face)
    left_sum = left_face + reoriented[:, prev_pos]
    right_sum = right_face + jnp.take_along_axis(left_face[:, next_pos], face_map[None, :, :], axis=2)
    local_out = put_face(local_out, left_sum, 0)
    local_out = put_face(local_out, right_sum, P_SIZE - 1)
    top_face = local_out[:, :, EZ - 1, :, P_SIZE - 1, :, :]
    bottom_face = local_out[:, :, 0, :, 0, :, :]
    top_sum = top_face + jnp.roll(bottom_face, -1, axis=0)
    bottom_sum = bottom_face + jnp.roll(top_face, 1, axis=0)
    local_out = local_out.at[:, :, 0, :, 0, :, :].set(bottom_sum)
    local_out = local_out.at[:, :, EZ - 1, :, P_SIZE - 1, :, :].set(top_sum)
    return local_out.reshape(LAYERS, SLABS, EZ, EY, PTS)
```

```python
import functools

import jax
import jax.numpy as jnp
import numpy as np
from jax import lax
from jax.experimental import pallas as pl
from jax.experimental.pallas import tpu as pltpu
from jax.sharding import PartitionSpec as P

P_SIZE = 8
PTS = 512
EY = 4
EZ = 4
CHUNK = 8
F32 = jnp.float32
BF16 = jnp.bfloat16
MESH = pl.DeviceIdType.MESH


def legendre_pair(gll_nodes, degree):
    lower_poly = gll_nodes * 0.0 + 1.0
    upper_poly = gll_nodes.copy()
    for poly_order in range(2, degree + 1):
        lower_poly, upper_poly = (
            upper_poly,
            ((2 * poly_order - 1) * gll_nodes * upper_poly - (poly_order - 1) * lower_poly)
            / poly_order,
        )
    return (lower_poly, upper_poly)


def gll_tables():
    degree = P_SIZE - 1
    gll_nodes = -np.cos(np.pi * np.arange(P_SIZE) / degree)
    for newton_sweep in range(100):
        lower_poly, upper_poly = legendre_pair(gll_nodes, degree)
        gll_nodes = gll_nodes - (gll_nodes * upper_poly - lower_poly) / ((degree + 1) * upper_poly)
    lower_poly, upper_poly = legendre_pair(gll_nodes, degree)
    quad_weights = 2.0 / (degree * (degree + 1) * upper_poly * upper_poly)
    identity = np.eye(P_SIZE)
    differ = gll_nodes[:, None] - gll_nodes[None, :] + identity
    derivative = upper_poly[:, None] / (upper_poly[None, :] * differ)
    derivative = derivative * (1.0 - identity)
    derivative[0, 0] = -degree * (degree + 1) / 4.0
    derivative[degree, degree] = degree * (degree + 1) / 4.0
    return derivative, quad_weights


def parts(table):
    high = np.asarray(table, np.float32).astype(BF16)
    low = (table - high.astype(np.float64)).astype(np.float32).astype(BF16)
    return high, low


def constant_tables():
    derivative, rho = gll_tables()
    eye = np.eye(P_SIZE)
    pair = np.eye(2)
    x_in = np.kron(pair, np.kron(eye, derivative.T))
    y_in = np.kron(pair, np.kron(derivative.T, eye))
    x_out = np.kron(pair, np.kron(eye, derivative))
    y_out = np.kron(pair, np.kron(derivative, eye))
    high, low = parts(np.concatenate([x_in, y_in], 1))
    matrices = [np.concatenate([part, part], 0) for part in (high, low)]
    for table in (x_out, y_out):
        both = np.concatenate(parts(table), 1)
        matrices.append(np.concatenate([both, both], 0))
    sub = np.arange(8)[:, None] // 4
    lane = np.arange(128)[None, :]
    c_low = 2 * sub + lane // 64
    vectors = []
    for table in (derivative, derivative.T):
        for sign in (1.0, -1.0):
            for move in (0, 2, 1, 3):
                other = c_low ^ move
                vectors.append((table[c_low, other] + sign * table[c_low, 7 - other]) / 2)
    plane = rho[lane // 8 % 8] * rho[lane % 8]
    for half in range(2):
        vectors.append(rho[4 * half + c_low] * plane)
    return np.stack(matrices), np.stack(vectors).astype(np.float32)


def turn(value, shift):
    return pltpu.roll(value, shift % 128, axis=value.ndim - 1) if shift % 128 else value


def slide(value, shift):
    return pltpu.roll(value, shift % 8, axis=value.ndim - 2)


def mirror(value):
    return slide(turn(value, 64), 4)


def iotas():
    sub = lax.broadcasted_iota(jnp.int32, (8, 128), 0)
    lane = lax.broadcasted_iota(jnp.int32, (8, 128), 1)
    return sub, lane


def split(value):
    high = value.astype(BF16)
    low = (value - high.astype(F32)).astype(BF16)
    return jnp.concatenate([high, low], axis=-1)


def along_z(low, high, table_ref, start):
    back = mirror(high)
    halves = []
    for value, first in ((low + back, start), (low - back, start + 4)):
        moved = slide(value, 4)
        total = table_ref[first] * value + table_ref[first + 1] * moved
        total += table_ref[first + 2] * turn(value, 64) + table_ref[first + 3] * turn(moved, 64)
        halves.append(total)
    even, odd = halves
    return even + odd, mirror(odd - even)


def flip_faces(value, sub, lane):
    value = jnp.take_along_axis(value, sub ^ 3, axis=0)
    return jnp.take_along_axis(value, lane ^ 56, axis=1)


def edge_mask(sub, lane, slot):
    base = jnp.where(sub < 4, 0, 71)
    return ((lane - base - slot) & 71) == 0


def chunk_local(u_ref, m_ref, mat_ref, vec_ref, flip_mask, sub, lane):
    count = u_ref.shape[0]
    rows = count * EZ * 2 * 8
    u = u_ref[...].reshape(rows, 128)
    both = split(u)
    grads = jnp.dot(both, mat_ref[0], preferred_element_type=F32)
    grads += jnp.dot(both, mat_ref[1], preferred_element_type=F32)
    weights = [vec_ref[16], vec_ref[17]]
    flux_x, flux_y, out_z = [], [], []
    for s in range(count):
        for ez in range(EZ):
            at = (s * EZ + ez) * 16
            pieces = along_z(u_ref[s, ez, 0], u_ref[s, ez, 1], vec_ref, 0)
            flux_z = [pieces[h] * (weights[h] * m_ref[s, ez, 2, h]) for h in range(2)]
            out_z.append(along_z(flux_z[0], flux_z[1], vec_ref, 8))
            for h in range(2):
                grad = grads[at + 8 * h : at + 8 * h + 8]
                flux_x.append(grad[:, :128] * (weights[h] * m_ref[s, ez, 0, h]))
                flux_y.append(grad[:, 128:] * (weights[h] * m_ref[s, ez, 1, h]))
    result = jnp.dot(split(jnp.concatenate(flux_x, 0)), mat_ref[2], preferred_element_type=F32)
    result += jnp.dot(split(jnp.concatenate(flux_y, 0)), mat_ref[3], preferred_element_type=F32)

    b = (lane >> 3) & 7
    a = lane & 7
    ey = sub & 3
    high_b = (b == 7) & (ey < 3)
    low_b = (b == 0) & (ey > 0)
    bottom = (sub < 4) & (lane < 64)
    top = (sub >= 4) & (lane >= 64)
    diagonal = bottom | top
    local, lefts, rights, z_own = [], [], [], []
    for s in range(count):
        block = []
        for ez in range(EZ):
            for h in range(2):
                at = (s * EZ + ez) * 16 + 8 * h
                v = result[at : at + 8, :128] + result[at : at + 8, 128:] + out_z[s * EZ + ez][h]
                after = turn(slide(v, -1), 56)
                before = turn(slide(v, 1), -56)
                block.append(v + jnp.where(high_b, after, jnp.where(low_b, before, 0.0)))
        for ez in range(EZ - 1):
            upper, lower = block[2 * ez + 1], block[2 * ez + 2]
            total = mirror(upper) + lower
            block[2 * ez + 2] = jnp.where(bottom, total, lower)
            block[2 * ez + 1] = jnp.where(top, mirror(total), upper)
        left, right = block[0], turn(block[7], 0)
        for j in range(1, 8):
            left = jnp.where(a == j, turn(block[j], j), left)
        for j in range(7):
            right = jnp.where(a == j, turn(block[j], j - 7), right)
        right = jnp.where(flip_mask(s), flip_faces(right, sub, lane), right)
        local.append(block)
        lefts.append(left)
        rights.append(right)
        z_own.append(jnp.where(bottom, block[0], block[7]))
    z_pairs = [
        jnp.where(diagonal, z_own[s], turn(z_own[s + 1], 64)) for s in range(0, count, 2)
    ]
    edges = []
    for faces in (lefts, rights):
        packed = faces[0]
        for s in range(1, count):
            packed = jnp.where(edge_mask(sub, lane, s), turn(faces[s], s), packed)
        moved = slide(packed, 4)
        edges.append(jnp.where(sub < 4, turn(moved, -71), turn(moved, 71)))
    return local, lefts, rights, z_pairs, edges


def chunk_final(local_ref, left_in, right_in, z_in, put):
    sub, lane = iotas()
    a = lane & 7
    bottom = (sub < 4) & (lane < 64)
    top = (sub >= 4) & (lane >= 64)
    count = local_ref.shape[0]
    for s in range(count):
        left, right, z = left_in(s), right_in(s), z_in(s)
        for j in range(8):
            v = local_ref[s, j // 2, j % 2]
            v += jnp.where(a == 0, turn(left, -j), jnp.where(a == 7, turn(right, 7 - j), 0.0))
            if j == 0:
                v += jnp.where(bottom, z, 0.0)
            if j == 7:
                v += jnp.where(top, z, 0.0)
            put(s, j, v)


def compute_kernel(u_ref, m_ref, mat_ref, vec_ref, fm_ref, ids_ref, local_ref, left_ref, right_ref, z_ref, el_ref, er_ref, inv_ref):
    step = pl.program_id(0)
    sub, lane = iotas()
    cycle = lax.axis_size("slab")
    device = lax.axis_index("slab")
    here = pl.num_programs(0) * CHUNK
    after = lax.rem(device + 1, cycle) * here
    before = lax.rem(device + cycle - 1, cycle) * here
    shift = cycle.bit_length() - 1
    for t in range(CHUNK):
        place = step * CHUNK + t
        inv_ref[ids_ref[before + place] >> shift] = place
        inv_ref[here + (ids_ref[after + place] >> shift)] = place

    def flip_mask(s):
        return fm_ref[s : s + 1, :] != lane

    local, lefts, rights, z_pairs, edges = chunk_local(
        u_ref, m_ref, mat_ref, vec_ref, flip_mask, sub, lane
    )
    for s in range(CHUNK):
        for j in range(8):
            local_ref[s, j // 2, j % 2] = local[s][j]
        left_ref[s] = lefts[s]
        right_ref[s] = rights[s]
    for s in range(CHUNK // 2):
        z_ref[s] = z_pairs[s]
    el_ref[0] = edges[0]
    er_ref[0] = edges[1]


def exchange_kernel(left, right, z, el, er, left_in, right_in, z_in, el_in, er_in, send_sem, recv_sem):
    cycle = lax.axis_size("slab")
    me = lax.axis_index("slab")
    layer = lax.axis_index("layer")
    after, before = lax.rem(me + 1, cycle), lax.rem(me + cycle - 1, cycle)
    other = 1 - layer
    peers = [(after, layer), (before, layer), (me, other), (after, other), (before, other)]
    barrier = pltpu.get_barrier_semaphore()
    for s, l in peers:
        pl.semaphore_signal(barrier, inc=1, device_id={"slab": s, "layer": l}, device_id_type=MESH)
    pl.semaphore_wait(barrier, 5)
    jobs = [(right, right_in), (left, left_in), (z, z_in), (er, er_in), (el, el_in)]
    copies = []
    for i, ((src, dst), (s, l)) in enumerate(zip(jobs, peers)):
        copies.append(
            pltpu.make_async_remote_copy(
                src_ref=src,
                dst_ref=dst,
                send_sem=send_sem.at[i],
                recv_sem=recv_sem.at[i],
                device_id={"slab": s, "layer": l},
                device_id_type=MESH,
            )
        )
    for copy in copies:
        copy.start()
    for copy in copies:
        copy.wait()


def final_kernel(local_ref, left_in, right_in, z_in, el_in, er_in, fm_ref, ids_ref, inv_ref, out_ref):
    step = pl.program_id(0)
    sub, lane = iotas()
    cycle = lax.axis_size("slab")
    device = lax.axis_index("slab")
    here = pl.num_programs(0) * CHUNK
    total = cycle * here
    shift = cycle.bit_length() - 1
    own = device * here + step * CHUNK
    on_edge = edge_mask(sub, lane, 0)

    def fetch(face_ref, edge_ref, at):
        packed = pltpu.roll(edge_ref[at >> 3], (128 - (at & 7)) & 127, axis=1)
        return face_ref[at] + jnp.where(on_edge, packed, 0.0)

    def get_left(s):
        at = inv_ref[lax.rem(ids_ref[own + s] + total - 1, total) >> shift]
        return fetch(right_in, er_in, at)

    def get_right(s):
        at = inv_ref[here + (lax.rem(ids_ref[own + s] + 1, total) >> shift)]
        value = fetch(left_in, el_in, at)
        return jnp.where(fm_ref[s : s + 1, :] != lane, flip_faces(value, sub, lane), value)

    def get_z(s):
        value = slide(z_in[s // 2], 4)
        return value if s % 2 else turn(value, 64)

    def put(s, j, value):
        out_ref[s, j // 2, j % 2] = value

    chunk_final(local_ref, get_left, get_right, get_z, put)


def body(nodal_field, metric, slab_ids, face_map):
    count = nodal_field.shape[1]
    steps = count // CHUNK
    u = nodal_field.reshape(count, EZ, EY, 2, 2, 128).transpose(0, 1, 3, 4, 2, 5)
    u = u.reshape(count, EZ, 2, 8, 128)
    m = metric.reshape(count, EZ, EY, 3, 2, 2, 128).transpose(0, 1, 3, 4, 5, 2, 6)
    m = m.reshape(count, EZ, 3, 2, 8, 128)
    matrices, vectors = constant_tables()
    matrices, vectors = jnp.asarray(matrices), jnp.asarray(vectors)
    smem = pl.BlockSpec(memory_space=pltpu.SMEM)
    vmem = pl.BlockSpec(memory_space=pltpu.VMEM)
    blocks = pl.BlockSpec((CHUNK, EZ, 2, 8, 128), lambda i: (i, 0, 0, 0, 0))
    faces = pl.BlockSpec((CHUNK, 8, 128), lambda i: (i, 0, 0))
    z_faces = pl.BlockSpec((CHUNK // 2, 8, 128), lambda i: (i, 0, 0))
    edges = pl.BlockSpec((1, 8, 128), lambda i: (i, 0, 0))
    fm_spec = pl.BlockSpec((CHUNK, 128), lambda i: (i, 0))
    shape = jax.ShapeDtypeStruct
    face_shape = shape((count, 8, 128), F32)
    z_shape = shape((count // 2, 8, 128), F32)
    edge_shape = shape((steps, 8, 128), F32)
    local, left, right, z, el, er, inv = pl.pallas_call(
        compute_kernel,
        grid=(steps,),
        in_specs=[
            blocks,
            pl.BlockSpec((CHUNK, EZ, 3, 2, 8, 128), lambda i: (i, 0, 0, 0, 0, 0)),
            vmem,
            vmem,
            fm_spec,
            smem,
        ],
        out_specs=[blocks, faces, faces, z_faces, edges, edges, smem],
        out_shape=[
            shape((count, EZ, 2, 8, 128), F32),
            face_shape,
            face_shape,
            z_shape,
            edge_shape,
            edge_shape,
            shape((2 * count,), jnp.int32),
        ],
    )(u, m, matrices, vectors, face_map, slab_ids)
    left_in, right_in, z_in, el_in, er_in = pl.pallas_call(
        exchange_kernel,
        in_specs=[vmem] * 5,
        out_specs=[vmem] * 5,
        out_shape=[face_shape, face_shape, z_shape, edge_shape, edge_shape],
        scratch_shapes=[pltpu.SemaphoreType.DMA((5,)), pltpu.SemaphoreType.DMA((5,))],
        compiler_params=pltpu.CompilerParams(collective_id=0, has_side_effects=True),
    )(left, right, z, el, er)
    out = pl.pallas_call(
        final_kernel,
        grid=(steps,),
        in_specs=[blocks, vmem, vmem, z_faces, vmem, vmem, fm_spec, smem, smem],
        out_specs=blocks,
        out_shape=shape((count, EZ, 2, 8, 128), F32),
    )(local, left_in, right_in, z_in, el_in, er_in, face_map, slab_ids, inv)
    out = out.reshape(count, EZ, 2, 2, EY, 128).transpose(0, 1, 4, 2, 3, 5)
    return out.reshape(1, count, EZ, EY, PTS)


def solution(mesh):
    return jax.shard_map(
        body,
        mesh=mesh,
        in_specs=(
            P("layer", "slab", None, None, None),
            P("layer", "slab", None, None, None, None),
            P(),
            P("slab", None),
        ),
        out_specs=P("layer", "slab", None, None, None),
        check_vma=False,
    )
```

```python
import functools

import jax
import jax.numpy as jnp
import numpy as np
from jax import lax
from jax.experimental import pallas as pl
from jax.experimental.pallas import tpu as pltpu
from jax.sharding import PartitionSpec as P

P_SIZE = 8
PTS = 512
EY = 4
EZ = 4
CHUNK = 8
F32 = jnp.float32
BF16 = jnp.bfloat16
MESH = pl.DeviceIdType.MESH


def legendre_pair(gll_nodes, degree):
    lower_poly = gll_nodes * 0.0 + 1.0
    upper_poly = gll_nodes.copy()
    for poly_order in range(2, degree + 1):
        lower_poly, upper_poly = (
            upper_poly,
            ((2 * poly_order - 1) * gll_nodes * upper_poly - (poly_order - 1) * lower_poly)
            / poly_order,
        )
    return (lower_poly, upper_poly)


def gll_tables():
    degree = P_SIZE - 1
    gll_nodes = -np.cos(np.pi * np.arange(P_SIZE) / degree)
    for newton_sweep in range(100):
        lower_poly, upper_poly = legendre_pair(gll_nodes, degree)
        gll_nodes = gll_nodes - (gll_nodes * upper_poly - lower_poly) / ((degree + 1) * upper_poly)
    lower_poly, upper_poly = legendre_pair(gll_nodes, degree)
    quad_weights = 2.0 / (degree * (degree + 1) * upper_poly * upper_poly)
    identity = np.eye(P_SIZE)
    differ = gll_nodes[:, None] - gll_nodes[None, :] + identity
    derivative = upper_poly[:, None] / (upper_poly[None, :] * differ)
    derivative = derivative * (1.0 - identity)
    derivative[0, 0] = -degree * (degree + 1) / 4.0
    derivative[degree, degree] = degree * (degree + 1) / 4.0
    return derivative, quad_weights


def parts(table):
    high = np.asarray(table, np.float32).astype(BF16)
    low = (table - high.astype(np.float64)).astype(np.float32).astype(BF16)
    return high, low


def constant_tables():
    derivative, rho = gll_tables()
    eye = np.eye(P_SIZE)
    pair = np.eye(2)
    x_in = np.kron(pair, np.kron(eye, derivative.T))
    y_in = np.kron(pair, np.kron(derivative.T, eye))
    x_out = np.kron(pair, np.kron(eye, derivative))
    y_out = np.kron(pair, np.kron(derivative, eye))
    high, low = parts(np.concatenate([x_in, y_in], 1))
    matrices = [high, low]
    for table in (x_out, y_out):
        matrices.append(np.concatenate(parts(table), 1))
    sub = np.arange(8)[:, None] // 4
    lane = np.arange(128)[None, :]
    c_low = 2 * sub + lane // 64
    vectors = []
    for table in (derivative, derivative.T):
        for half in range(2):
            for source in range(2):
                for move in (0, 2, 1, 3):
                    vectors.append(table[4 * half + c_low, 4 * source + (c_low ^ move)])
    plane = rho[lane // 8 % 8] * rho[lane % 8]
    for half in range(2):
        vectors.append(rho[4 * half + c_low] * plane)
    return np.stack(matrices), np.stack(vectors).astype(np.float32)


def turn(value, shift):
    return pltpu.roll(value, shift % 128, axis=value.ndim - 1) if shift % 128 else value


def slide(value, shift):
    return pltpu.roll(value, shift % 8, axis=value.ndim - 2)


def mirror(value):
    return slide(turn(value, 64), 4)


def iotas():
    sub = lax.broadcasted_iota(jnp.int32, (8, 128), 0)
    lane = lax.broadcasted_iota(jnp.int32, (8, 128), 1)
    return sub, lane


def split(value):
    high = value.astype(BF16)
    low = (value - high.astype(F32)).astype(BF16)
    return jnp.concatenate([high, low], axis=-1)


def product(both, matrix):
    return jnp.dot(both, jnp.concatenate([matrix, matrix], 0), preferred_element_type=F32)


def along_z(low, high, low_turned, high_turned, table_ref, start):
    terms = []
    for value, turned in ((low, low_turned), (high, high_turned)):
        terms += [value, slide(value, 4), turned, slide(turned, 4)]
    out = []
    for half in range(2):
        total = table_ref[start + 8 * half] * terms[0]
        for k in range(1, 8):
            total += table_ref[start + 8 * half + k] * terms[k]
        out.append(total)
    return out


def flip_faces(value, sub, lane):
    value = jnp.take_along_axis(value, sub ^ 3, axis=0)
    return jnp.take_along_axis(value, lane ^ 56, axis=1)


def edge_mask(sub, lane, slot):
    base = jnp.where(sub < 4, 0, 71)
    return ((lane - base - slot) & 71) == 0


def chunk_local(u_ref, m_ref, mat_ref, vec_ref, flip_mask, sub, lane):
    count = u_ref.shape[0]
    rows = count * EZ * 2 * 8
    u = u_ref[...].reshape(rows, 128)
    both = split(u)
    grads = product(both, mat_ref[0]) + product(both, mat_ref[1])
    weights = [vec_ref[32], vec_ref[33]]
    turned = turn(u, 64)
    flux_x, flux_y, flux_z = [], [], []
    for s in range(count):
        for ez in range(EZ):
            at = (s * EZ + ez) * 16
            pieces = along_z(
                u[at : at + 8], u[at + 8 : at + 16], turned[at : at + 8], turned[at + 8 : at + 16], vec_ref, 0
            )
            for h in range(2):
                grad = grads[at + 8 * h : at + 8 * h + 8]
                flux_z.append(pieces[h] * (weights[h] * m_ref[s, ez, 2, h]))
                flux_x.append(grad[:, :128] * (weights[h] * m_ref[s, ez, 0, h]))
                flux_y.append(grad[:, 128:] * (weights[h] * m_ref[s, ez, 1, h]))
    flux_turned = [turn(value, 64) for value in flux_z]
    out_z = [
        along_z(flux_z[k], flux_z[k + 1], flux_turned[k], flux_turned[k + 1], vec_ref, 16)
        for k in range(0, 2 * count * EZ, 2)
    ]
    result = product(split(jnp.concatenate(flux_x, 0)), mat_ref[2])
    result += product(split(jnp.concatenate(flux_y, 0)), mat_ref[3])

    b = (lane >> 3) & 7
    a = lane & 7
    ey = sub & 3
    high_b = (b == 7) & (ey < 3)
    low_b = (b == 0) & (ey > 0)
    bottom = (sub < 4) & (lane < 64)
    top = (sub >= 4) & (lane >= 64)
    diagonal = bottom | top
    local, lefts, rights, z_own = [], [], [], []
    for s in range(count):
        block = []
        for ez in range(EZ):
            for h in range(2):
                at = (s * EZ + ez) * 16 + 8 * h
                v = result[at : at + 8, :128] + result[at : at + 8, 128:] + out_z[s * EZ + ez][h]
                after = turn(slide(v, -1), 56)
                before = turn(slide(v, 1), -56)
                block.append(v + jnp.where(high_b, after, jnp.where(low_b, before, 0.0)))
        for ez in range(EZ - 1):
            upper, lower = block[2 * ez + 1], block[2 * ez + 2]
            block[2 * ez + 2] = jnp.where(bottom, lower + mirror(upper), lower)
            block[2 * ez + 1] = jnp.where(top, upper + mirror(lower), upper)
        left, right = block[0], turn(block[7], 0)
        for j in range(1, 8):
            left = jnp.where(a == j, turn(block[j], j), left)
        for j in range(7):
            right = jnp.where(a == j, turn(block[j], j - 7), right)
        right = jnp.where(flip_mask(s), flip_faces(right, sub, lane), right)
        local.append(block)
        lefts.append(left)
        rights.append(right)
        z_own.append(jnp.where(bottom, block[0], block[7]))
    z_pairs = [
        jnp.where(diagonal, z_own[s], turn(z_own[s + 1], 64)) for s in range(0, count, 2)
    ]
    edges = []
    for faces in (lefts, rights):
        packed = faces[0]
        for s in range(1, count):
            packed = jnp.where(edge_mask(sub, lane, s), turn(faces[s], s), packed)
        moved = slide(packed, 4)
        edges.append(jnp.where(sub < 4, turn(moved, -71), turn(moved, 71)))
    return local, lefts, rights, z_pairs, edges


def chunk_final(local_ref, left_in, right_in, z_in, put):
    sub, lane = iotas()
    a = lane & 7
    bottom = (sub < 4) & (lane < 64)
    top = (sub >= 4) & (lane >= 64)
    count = local_ref.shape[0]
    for s in range(count):
        left, right, z = left_in(s), right_in(s), z_in(s)
        for j in range(8):
            v = local_ref[s, j // 2, j % 2]
            v += jnp.where(a == 0, turn(left, -j), jnp.where(a == 7, turn(right, 7 - j), 0.0))
            if j == 0:
                v += jnp.where(bottom, z, 0.0)
            if j == 7:
                v += jnp.where(top, z, 0.0)
            put(s, j, v)


def positions(wanted, values, offset, count):
    t = lax.broadcasted_iota(jnp.int32, (count, 128), 0)
    lane = lax.broadcasted_iota(jnp.int32, (count, 128), 1)
    column = jnp.sum(jnp.where(lane == t + offset, values, 0).astype(F32), axis=1, keepdims=True)
    hit = column == wanted.astype(F32)
    return jnp.sum(jnp.where(hit, t, 0).astype(F32), axis=0, keepdims=True).astype(jnp.int32)


def main_kernel(
    u_hbm, m_hbm, mat_hbm, vec_hbm, fm_hbm, ids_hbm,
    local, left_in, right_in, z_in, el_in, er_in, fm, pos,
    u_v, m_v, mat, vec, ids, pos_v, left, right, z, el, er,
    in_sem, one_sem, send_sem, recv_sem,
):
    cycle = lax.axis_size("slab")
    me = lax.axis_index("slab")
    layer = lax.axis_index("layer")
    after, before = lax.rem(me + 1, cycle), lax.rem(me + cycle - 1, cycle)
    other = 1 - layer
    peers = [(after, layer), (before, layer), (me, other), (after, other), (before, other)]
    count = local.shape[0]
    steps = count // CHUNK
    total = cycle * count
    barrier = pltpu.get_barrier_semaphore()
    for s, l in peers:
        pl.semaphore_signal(barrier, inc=1, device_id={"slab": s, "layer": l}, device_id_type=MESH)

    def loads(i):
        part = pl.ds(i * CHUNK, CHUNK)
        return [
            pltpu.make_async_copy(u_hbm.at[part], u_v.at[part], in_sem.at[0, i]),
            pltpu.make_async_copy(m_hbm.at[part], m_v.at[part], in_sem.at[1, i]),
        ]

    def once():
        pairs = [(mat_hbm, mat), (vec_hbm, vec), (fm_hbm.at[:, pl.ds(0, 128)], fm), (ids_hbm, ids)]
        return [pltpu.make_async_copy(a, b, one_sem.at[k]) for k, (a, b) in enumerate(pairs)]

    for copy in loads(0) + once():
        copy.start()
    for i in range(1, steps):
        for copy in loads(i):
            copy.start()
    for copy in once():
        copy.wait()

    per_row = 128 // count
    rows = [ids[pl.ds(d // per_row, 1), :] for d in (me, before, after)]
    sub, lane = iotas()
    found = []
    for row, device, move in ((rows[1], before, total - 1), (rows[2], after, 1)):
        wanted = rows[0] + move
        wanted = jnp.where(wanted >= total, wanted - total, wanted)
        found.append(positions(wanted, row, lax.rem(device, per_row) * count, count))
    pos_v[...] = jnp.where(sub == 0, found[0], found[1])
    pos_copy = pltpu.make_async_copy(pos_v, pos, one_sem.at[4])
    pos_copy.start()

    def sends(i, chunks):
        part = pl.ds(i * CHUNK, chunks * CHUNK)
        half = pl.ds(i * (CHUNK // 2), chunks * (CHUNK // 2))
        single = pl.ds(i, chunks)
        jobs = [(right, right_in, part), (left, left_in, part), (z, z_in, half), (er, er_in, single), (el, el_in, single)]
        return [
            pltpu.make_async_remote_copy(
                src_ref=src.at[at],
                dst_ref=dst.at[at],
                send_sem=send_sem.at[k],
                recv_sem=recv_sem.at[k],
                device_id={"slab": s, "layer": l},
                device_id_type=MESH,
            )
            for k, ((src, dst, at), (s, l)) in enumerate(zip(jobs, peers))
        ]

    pl.semaphore_wait(barrier, 5)

    def step(i, carry):
        for copy in loads(i):
            copy.wait()

        def flip_mask(s):
            return fm[pl.ds(i * CHUNK + s, 1), :] != lane

        blocks, lefts, rights, z_pairs, edges = chunk_local(
            u_v.at[pl.ds(i * CHUNK, CHUNK)], m_v.at[pl.ds(i * CHUNK, CHUNK)], mat, vec, flip_mask, sub, lane
        )
        for s in range(CHUNK):
            for j in range(8):
                local[i * CHUNK + s, j // 2, j % 2] = blocks[s][j]
            left[i * CHUNK + s] = lefts[s]
            right[i * CHUNK + s] = rights[s]
        for s in range(CHUNK // 2):
            z[i * (CHUNK // 2) + s] = z_pairs[s]
        el[i] = edges[0]
        er[i] = edges[1]
        for copy in sends(i, 1):
            copy.start()
        return carry

    lax.fori_loop(0, steps, step, 0)

    pos_copy.wait()
    for copy in sends(0, steps):
        copy.wait()


def final_kernel(local, left_in, right_in, z_in, el_in, er_in, fm, pos, out_hbm, out, sem):
    sub, lane = iotas()
    count = local.shape[0]
    steps = count // CHUNK
    per_row = 128 // count
    first = lax.rem(lax.axis_index("slab"), per_row) * count
    on_edge = edge_mask(sub, lane, 0)

    def write(i):
        part = pl.ds(i * CHUNK, CHUNK)
        return pltpu.make_async_copy(out.at[part], out_hbm.at[part], sem.at[i])

    def fetch(face_ref, edge_ref, at):
        packed = pltpu.roll(edge_ref[at >> 3], (128 - (at & 7)) & 127, axis=1)
        return face_ref[at] + jnp.where(on_edge, packed, 0.0)

    def step(i, carry):
        base = i * CHUNK

        def get_left(s):
            return fetch(right_in, er_in, pos[0, first + base + s])

        def get_right(s):
            value = fetch(left_in, el_in, pos[1, first + base + s])
            return jnp.where(fm[pl.ds(base + s, 1), :] != lane, flip_faces(value, sub, lane), value)

        def get_z(s):
            value = slide(z_in[i * (CHUNK // 2) + s // 2], 4)
            return value if s % 2 else turn(value, 64)

        def put(s, j, value):
            out[base + s, j // 2, j % 2] = value

        chunk_final(local.at[pl.ds(base, CHUNK)], get_left, get_right, get_z, put)
        write(i).start()
        return carry

    lax.fori_loop(0, steps, step, 0)

    def finish(i, carry):
        write(i).wait()
        return carry

    lax.fori_loop(0, steps, finish, 0)


def body(nodal_field, metric, slab_ids, face_map):
    count = nodal_field.shape[1]
    steps = count // CHUNK
    u = nodal_field.reshape(count, EZ, EY, 2, 2, 128).transpose(0, 1, 3, 4, 2, 5)
    u = u.reshape(count, EZ, 2, 8, 128)
    m = metric.reshape(count, EZ, EY, 3, 2, 2, 128).transpose(0, 1, 3, 4, 5, 2, 6)
    m = m.reshape(count, EZ, 3, 2, 8, 128)
    ids = slab_ids.reshape(-1, 128)
    matrices, vectors = constant_tables()
    matrices, vectors = jnp.asarray(matrices), jnp.asarray(vectors)
    hbm = pl.BlockSpec(memory_space=pltpu.HBM)
    vmem = pl.BlockSpec(memory_space=pltpu.VMEM)
    smem = pl.BlockSpec(memory_space=pltpu.SMEM)
    whole = (count, EZ, 2, 8, 128)
    face, z_face, edge = (count, 8, 128), (count // 2, 8, 128), (steps, 8, 128)
    dma = pltpu.SemaphoreType.DMA
    shared = pl.pallas_call(
        main_kernel,
        in_specs=[hbm] * 6,
        out_specs=[vmem] * 7 + [smem],
        out_shape=[pltpu.VMEM(s, F32) for s in (whole, face, face, z_face, edge, edge)]
        + [pltpu.VMEM((count, 128), jnp.int32), pltpu.SMEM((8, 128), jnp.int32)],
        scratch_shapes=[
            pltpu.VMEM(u.shape, F32),
            pltpu.VMEM(m.shape, F32),
            pltpu.VMEM(matrices.shape, BF16),
            pltpu.VMEM(vectors.shape, F32),
            pltpu.VMEM(ids.shape, jnp.int32),
            pltpu.VMEM((8, 128), jnp.int32),
            pltpu.VMEM(face, F32),
            pltpu.VMEM(face, F32),
            pltpu.VMEM(z_face, F32),
            pltpu.VMEM(edge, F32),
            pltpu.VMEM(edge, F32),
            dma((2, steps)),
            dma((5,)),
            dma((5,)),
            dma((5,)),
        ],
        compiler_params=pltpu.CompilerParams(
            collective_id=0, has_side_effects=True, vmem_limit_bytes=60 * 2**20
        ),
    )(u, m, matrices, vectors, face_map, ids)
    out = pl.pallas_call(
        final_kernel,
        in_specs=[vmem] * 7 + [smem],
        out_specs=hbm,
        out_shape=jax.ShapeDtypeStruct(whole, F32),
        scratch_shapes=[pltpu.VMEM(whole, F32), dma((steps,))],
        compiler_params=pltpu.CompilerParams(vmem_limit_bytes=40 * 2**20),
    )(*shared)
    out = out.reshape(count, EZ, 2, 2, EY, 128).transpose(0, 1, 4, 2, 3, 5)
    return out.reshape(1, count, EZ, EY, PTS)


def solution(mesh):
    return jax.shard_map(
        body,
        mesh=mesh,
        in_specs=(
            P("layer", "slab", None, None, None),
            P("layer", "slab", None, None, None, None),
            P(),
            P("slab", None),
        ),
        out_specs=P("layer", "slab", None, None, None),
        check_vma=False,
    )
```

```python
import functools

import jax
import jax.numpy as jnp
import numpy as np
from jax import lax
from jax.experimental import pallas as pl
from jax.experimental.pallas import tpu as pltpu
from jax.sharding import PartitionSpec as P

P_SIZE = 8
PTS = 512
EY = 4
EZ = 4
CHUNK = 8
LAST = 16
GATHER = 16
F32 = jnp.float32
BF16 = jnp.bfloat16
MESH = pl.DeviceIdType.MESH


def legendre_pair(gll_nodes, degree):
    lower_poly = gll_nodes * 0.0 + 1.0
    upper_poly = gll_nodes.copy()
    for poly_order in range(2, degree + 1):
        lower_poly, upper_poly = (
            upper_poly,
            ((2 * poly_order - 1) * gll_nodes * upper_poly - (poly_order - 1) * lower_poly)
            / poly_order,
        )
    return (lower_poly, upper_poly)


def gll_tables():
    degree = P_SIZE - 1
    gll_nodes = -np.cos(np.pi * np.arange(P_SIZE) / degree)
    for newton_sweep in range(100):
        lower_poly, upper_poly = legendre_pair(gll_nodes, degree)
        gll_nodes = gll_nodes - (gll_nodes * upper_poly - lower_poly) / ((degree + 1) * upper_poly)
    lower_poly, upper_poly = legendre_pair(gll_nodes, degree)
    quad_weights = 2.0 / (degree * (degree + 1) * upper_poly * upper_poly)
    identity = np.eye(P_SIZE)
    differ = gll_nodes[:, None] - gll_nodes[None, :] + identity
    derivative = upper_poly[:, None] / (upper_poly[None, :] * differ)
    derivative = derivative * (1.0 - identity)
    derivative[0, 0] = -degree * (degree + 1) / 4.0
    derivative[degree, degree] = degree * (degree + 1) / 4.0
    return derivative, quad_weights


def parts(table):
    high = np.asarray(table, np.float32).astype(BF16)
    low = (table - high.astype(np.float64)).astype(np.float32).astype(BF16)
    return high, low


def constant_tables():
    derivative, rho = gll_tables()
    eye = np.eye(P_SIZE)
    pair = np.eye(2)
    x_in = np.kron(pair, np.kron(eye, derivative.T))
    y_in = np.kron(pair, np.kron(derivative.T, eye))
    x_out = np.kron(pair, np.kron(eye, derivative))
    y_out = np.kron(pair, np.kron(derivative, eye))
    high, low = parts(np.concatenate([x_in, y_in], 1))
    matrices = [high, low]
    for table in (x_out, y_out):
        matrices.append(np.concatenate(parts(table), 1))
    sub = np.arange(8)[:, None] // 4
    lane = np.arange(128)[None, :]
    c_low = 2 * sub + lane // 64
    vectors = []
    for table in (derivative, derivative.T):
        for half in range(2):
            for source in range(2):
                for move in (0, 2, 1, 3):
                    vectors.append(table[4 * half + c_low, 4 * source + (c_low ^ move)])
    plane = rho[lane // 8 % 8] * rho[lane % 8]
    for half in range(2):
        vectors.append(rho[4 * half + c_low] * plane)
    return np.stack(matrices), np.stack(vectors).astype(np.float32)


def turn(value, shift):
    return pltpu.roll(value, shift % 128, axis=value.ndim - 1) if shift % 128 else value


def slide(value, shift):
    return pltpu.roll(value, shift % 8, axis=value.ndim - 2)


def mirror(value):
    return slide(turn(value, 64), 4)


def iotas():
    sub = lax.broadcasted_iota(jnp.int32, (8, 128), 0)
    lane = lax.broadcasted_iota(jnp.int32, (8, 128), 1)
    return sub, lane


def split(value):
    high = value.astype(BF16)
    low = (value - high.astype(F32)).astype(BF16)
    return jnp.concatenate([high, low], axis=-1)


def product(both, matrix):
    return jnp.dot(both, jnp.concatenate([matrix, matrix], 0), preferred_element_type=F32)


def along_z(low, high, low_turned, high_turned, table_ref, start):
    terms = []
    for value, turned in ((low, low_turned), (high, high_turned)):
        terms += [value, slide(value, 4), turned, slide(turned, 4)]
    out = []
    for half in range(2):
        total = table_ref[start + 8 * half] * terms[0]
        for k in range(1, 8):
            total += table_ref[start + 8 * half + k] * terms[k]
        out.append(total)
    return out


def flip_faces(value, sub, lane, shift):
    value = jnp.take_along_axis(value, sub ^ 3, axis=0)
    return jnp.take_along_axis(value, ((((lane - shift) & 127) ^ 56) + shift) & 127, axis=1)


def edge_mask(sub, lane, slot):
    base = jnp.where(sub < 4, 0, 71)
    return ((lane - base - slot) & 71) == 0


def chunk_fluxes(u_ref, m_ref, mat_ref, vec_ref, fx_ref, fy_ref, fz_ref):
    count = u_ref.shape[0]
    rows = count * EZ * 2 * 8
    u = u_ref[...].reshape(rows, 128)
    both = split(u)
    grads = product(both, mat_ref[0]) + product(both, mat_ref[1])
    weights = [vec_ref[32], vec_ref[33]]
    turned = turn(u, 64)
    flux_x, flux_y = [], []
    for s in range(count):
        for ez in range(EZ):
            at = (s * EZ + ez) * 16
            pieces = along_z(
                u[at : at + 8], u[at + 8 : at + 16], turned[at : at + 8], turned[at + 8 : at + 16], vec_ref, 0
            )
            for h in range(2):
                grad = grads[at + 8 * h : at + 8 * h + 8]
                fz_ref[at // 8 + h] = pieces[h] * (weights[h] * m_ref[s, ez, 2, h])
                flux_x.append(grad[:, :128] * (weights[h] * m_ref[s, ez, 0, h]))
                flux_y.append(grad[:, 128:] * (weights[h] * m_ref[s, ez, 1, h]))
    fx_ref[...] = split(jnp.concatenate(flux_x, 0))
    fy_ref[...] = split(jnp.concatenate(flux_y, 0))


def chunk_local(fx_ref, fy_ref, fz_ref, mat_ref, vec_ref, flip_mask, sub, lane):
    count = CHUNK
    result = product(fx_ref[...], mat_ref[2]) + product(fy_ref[...], mat_ref[3])
    flux_z = [fz_ref[k] for k in range(2 * count * EZ)]
    flux_turned = [turn(value, 64) for value in flux_z]
    out_z = [
        along_z(flux_z[k], flux_z[k + 1], flux_turned[k], flux_turned[k + 1], vec_ref, 16)
        for k in range(0, 2 * count * EZ, 2)
    ]
    b = (lane >> 3) & 7
    a = lane & 7
    ey = sub & 3
    swap = jnp.where((b == 0) | (b == 7), lane ^ 56, lane)
    high_b = (b == 7) & (ey < 3)
    low_b = (b == 0) & (ey > 0)
    bottom = (sub < 4) & (lane < 64)
    top = (sub >= 4) & (lane >= 64)
    diagonal = bottom | top
    local, lefts, rights, z_own = [], [], [], []
    for s in range(count):
        block = []
        for ez in range(EZ):
            for h in range(2):
                at = (s * EZ + ez) * 16 + 8 * h
                v = result[at : at + 8, :128] + result[at : at + 8, 128:] + out_z[s * EZ + ez][h]
                swapped = jnp.take_along_axis(v, swap, axis=1)
                met = jnp.where(high_b, slide(swapped, -1), jnp.where(low_b, slide(swapped, 1), 0.0))
                block.append(v + met)
        for ez in range(EZ - 1):
            upper, lower = block[2 * ez + 1], block[2 * ez + 2]
            block[2 * ez + 2] = jnp.where(bottom, lower + mirror(upper), lower)
            block[2 * ez + 1] = jnp.where(top, upper + mirror(lower), upper)
        left = right = block[0]
        for j in range(1, 8):
            moved = turn(block[j], j)
            left = jnp.where(a == j, moved, left)
            right = jnp.where(a == j - 1, moved, right)
        right = jnp.where(flip_mask(s), flip_faces(right, sub, lane, 7), right)
        local.append(block)
        lefts.append(left)
        rights.append(right)
        z_own.append(jnp.where(bottom, block[0], block[7]))
    z_pairs = [
        jnp.where(diagonal, z_own[s], turn(z_own[s + 1], 64)) for s in range(0, count, 2)
    ]
    edges = []
    for faces, shift in ((lefts, 0), (rights, 7)):
        packed = faces[0]
        for s in range(1, count):
            packed = jnp.where(edge_mask(sub, lane, s + shift), turn(faces[s], s), packed)
        moved = slide(packed, 4)
        edges.append(jnp.where(sub < 4, turn(moved, -71 - shift), turn(moved, 71 - shift)))
    return local, lefts, rights, z_pairs, edges


def positions(wanted, values, offset, count):
    t = lax.broadcasted_iota(jnp.int32, (count, 128), 0)
    lane = lax.broadcasted_iota(jnp.int32, (count, 128), 1)
    column = jnp.sum(jnp.where(lane == t + offset, values, 0).astype(F32), axis=1, keepdims=True)
    hit = column == wanted.astype(F32)
    return jnp.sum(jnp.where(hit, t, 0).astype(F32), axis=0, keepdims=True).astype(jnp.int32)


def main_kernel(
    u_hbm, m_hbm, mat_hbm, vec_hbm, fm_hbm, ids_hbm,
    local, left_in, right_in, z_in, el_in, er_in, fm, pos,
    u_v, m_v, fx, fy, fz, mat, vec, ids, pos_v, left, right, z, el, er,
    in_sem, one_sem, send_sem, recv_sem,
):
    cycle = lax.axis_size("slab")
    me = lax.axis_index("slab")
    layer = lax.axis_index("layer")
    after, before = lax.rem(me + 1, cycle), lax.rem(me + cycle - 1, cycle)
    other = 1 - layer
    peers = [(after, layer), (before, layer), (me, other), (after, other), (before, other)]
    count = local.shape[0]
    steps = count // CHUNK
    total = cycle * count
    barrier = pltpu.get_barrier_semaphore()
    for s, l in peers:
        pl.semaphore_signal(barrier, inc=1, device_id={"slab": s, "layer": l}, device_id_type=MESH)

    def loads(i):
        part = pl.ds(i * CHUNK, CHUNK)
        return [
            pltpu.make_async_copy(u_hbm.at[part], u_v.at[part], in_sem.at[0, i]),
            pltpu.make_async_copy(m_hbm.at[part], m_v.at[part], in_sem.at[1, i]),
        ]

    def once():
        pairs = [(mat_hbm, mat), (vec_hbm, vec), (fm_hbm.at[:, pl.ds(0, 128)], fm), (ids_hbm, ids)]
        return [pltpu.make_async_copy(a, b, one_sem.at[k]) for k, (a, b) in enumerate(pairs)]

    for copy in loads(0) + once():
        copy.start()
    for i in range(1, steps):
        for copy in loads(i):
            copy.start()
    for copy in once():
        copy.wait()

    per_row = 128 // count
    rows = [ids[pl.ds(d // per_row, 1), :] for d in (me, before, after)]
    sub, lane = iotas()
    found = []
    for row, device, move in ((rows[1], before, total - 1), (rows[2], after, 1)):
        wanted = rows[0] + move
        wanted = jnp.where(wanted >= total, wanted - total, wanted)
        found.append(positions(wanted, row, lax.rem(device, per_row) * count, count))
    pos_v[...] = jnp.where(sub == 0, found[0], found[1])
    pos_copy = pltpu.make_async_copy(pos_v, pos, one_sem.at[4])
    pos_copy.start()

    def sends(i, chunks):
        part = pl.ds(i * CHUNK, chunks * CHUNK)
        half = pl.ds(i * (CHUNK // 2), chunks * (CHUNK // 2))
        single = pl.ds(i, chunks)
        jobs = [(right, right_in, part), (left, left_in, part), (z, z_in, half), (er, er_in, single), (el, el_in, single)]
        return [
            pltpu.make_async_remote_copy(
                src_ref=src.at[at],
                dst_ref=dst.at[at],
                send_sem=send_sem.at[k],
                recv_sem=recv_sem.at[k],
                device_id={"slab": s, "layer": l},
                device_id_type=MESH,
            )
            for k, ((src, dst, at), (s, l)) in enumerate(zip(jobs, peers))
        ]

    def fluxes(i):
        for copy in loads(i):
            copy.wait()
        part = pl.ds(i * CHUNK, CHUNK)
        chunk_fluxes(u_v.at[part], m_v.at[part], mat, vec, fx, fy, fz)

    def assemble(i):
        def flip_mask(s):
            return fm[pl.ds(i * CHUNK + s, 1), :] != lane

        blocks, lefts, rights, z_pairs, edges = chunk_local(fx, fy, fz, mat, vec, flip_mask, sub, lane)
        for s in range(CHUNK):
            for j in range(8):
                local[i * CHUNK + s, j // 2, j % 2] = blocks[s][j]
            left[i * CHUNK + s] = lefts[s]
            right[i * CHUNK + s] = rights[s]
        for s in range(CHUNK // 2):
            z[i * (CHUNK // 2) + s] = z_pairs[s]
        el[i] = edges[0]
        er[i] = edges[1]

    def launch(i):
        for copy in sends(i, 1):
            copy.start()

    fluxes(0)
    pl.semaphore_wait(barrier, 5)

    def step(i, carry):
        for copy in loads(i):
            copy.wait()
        assemble(i - 1)
        part = pl.ds(i * CHUNK, CHUNK)
        chunk_fluxes(u_v.at[part], m_v.at[part], mat, vec, fx, fy, fz)
        launch(i - 1)
        return carry

    lax.fori_loop(1, steps, step, 0)
    assemble(steps - 1)
    launch(steps - 1)
    pos_copy.wait()
    for copy in sends(0, steps):
        copy.wait()


def final_kernel(local, left_in, right_in, z_in, el_in, er_in, fm, pos, out_hbm, out, faces, sem):
    sub, lane = iotas()
    count = local.shape[0]
    per_row = 128 // count
    first = lax.rem(lax.axis_index("slab"), per_row) * count
    on_edge = edge_mask(sub, lane, 0)
    even = (lane & 1) == 0
    a = lane & 7
    on_face = (a == 0) | (a == 7)
    bottom = (sub < 4) & (lane < 64)
    top = (sub >= 4) & (lane >= 64)

    def write(i):
        part = pl.ds(i * LAST, LAST)
        return pltpu.make_async_copy(out.at[part], out_hbm.at[part], sem.at[i])

    def edge(edge_ref, at):
        return jnp.where(on_edge, pltpu.roll(edge_ref[at >> 3], (128 - (at & 7)) & 127, axis=1), 0.0)

    def gather(i, carry):
        for s in range(GATHER):
            slab = i * GATHER + s
            back, ahead = pos[0, first + slab], pos[1, first + slab]
            low = turn(right_in[back], -7) + edge(er_in, back)
            high = left_in[ahead] + edge(el_in, ahead)
            flipped = fm[pl.ds(slab, 1), :] != lane
            high = turn(jnp.where(flipped, flip_faces(high, sub, lane, 0), high), 7)
            faces[slab, 0] = jnp.where(even, low, high)
            faces[slab, 1] = jnp.where(even, high, low)
        return carry

    lax.fori_loop(0, count // GATHER, gather, 0)

    def step(i, carry):
        for s in range(LAST):
            slab = i * LAST + s
            z = slide(z_in[i * (LAST // 2) + s // 2], 4)
            z = z if s % 2 else turn(z, 64)
            for j in range(8):
                v = local[slab, j // 2, j % 2] + jnp.where(on_face, turn(faces[slab, j % 2], -j), 0.0)
                if j == 0:
                    v += jnp.where(bottom, z, 0.0)
                if j == 7:
                    v += jnp.where(top, z, 0.0)
                out[slab, j // 2, j % 2] = v
        write(i).start()
        return carry

    lax.fori_loop(0, count // LAST, step, 0)

    def finish(i, carry):
        write(i).wait()
        return carry

    lax.fori_loop(0, count // LAST, finish, 0)


def body(nodal_field, metric, slab_ids, face_map):
    count = nodal_field.shape[1]
    steps = count // CHUNK
    u = nodal_field.reshape(count, EZ, EY, 2, 2, 128).transpose(0, 1, 3, 4, 2, 5)
    u = u.reshape(count, EZ, 2, 8, 128)
    m = metric.reshape(count, EZ, EY, 3, 2, 2, 128).transpose(0, 1, 3, 4, 5, 2, 6)
    m = m.reshape(count, EZ, 3, 2, 8, 128)
    ids = slab_ids.reshape(-1, 128)
    matrices, vectors = constant_tables()
    matrices, vectors = jnp.asarray(matrices), jnp.asarray(vectors)
    hbm = pl.BlockSpec(memory_space=pltpu.HBM)
    vmem = pl.BlockSpec(memory_space=pltpu.VMEM)
    smem = pl.BlockSpec(memory_space=pltpu.SMEM)
    whole = (count, EZ, 2, 8, 128)
    face, z_face, edge = (count, 8, 128), (count // 2, 8, 128), (steps, 8, 128)
    dma = pltpu.SemaphoreType.DMA
    shared = pl.pallas_call(
        main_kernel,
        in_specs=[hbm] * 6,
        out_specs=[vmem] * 7 + [smem],
        out_shape=[pltpu.VMEM(s, F32) for s in (whole, face, face, z_face, edge, edge)]
        + [pltpu.VMEM((count, 128), jnp.int32), pltpu.SMEM((8, 128), jnp.int32)],
        scratch_shapes=[
            pltpu.VMEM(u.shape, F32),
            pltpu.VMEM(m.shape, F32),
            pltpu.VMEM((CHUNK * EZ * 16, 256), BF16),
            pltpu.VMEM((CHUNK * EZ * 16, 256), BF16),
            pltpu.VMEM((CHUNK * EZ * 2, 8, 128), F32),
            pltpu.VMEM(matrices.shape, BF16),
            pltpu.VMEM(vectors.shape, F32),
            pltpu.VMEM(ids.shape, jnp.int32),
            pltpu.VMEM((8, 128), jnp.int32),
            pltpu.VMEM(face, F32),
            pltpu.VMEM(face, F32),
            pltpu.VMEM(z_face, F32),
            pltpu.VMEM(edge, F32),
            pltpu.VMEM(edge, F32),
            dma((2, steps)),
            dma((5,)),
            dma((5,)),
            dma((5,)),
        ],
        compiler_params=pltpu.CompilerParams(
            collective_id=0, has_side_effects=True, vmem_limit_bytes=60 * 2**20
        ),
    )(u, m, matrices, vectors, face_map, ids)
    out = pl.pallas_call(
        final_kernel,
        in_specs=[vmem] * 7 + [smem],
        out_specs=hbm,
        out_shape=jax.ShapeDtypeStruct(whole, F32),
        scratch_shapes=[pltpu.VMEM(whole, F32), pltpu.VMEM((count, 2, 8, 128), F32), dma((count // LAST,))],
        compiler_params=pltpu.CompilerParams(vmem_limit_bytes=40 * 2**20),
    )(*shared)
    out = out.reshape(count, EZ, 2, 2, EY, 128).transpose(0, 1, 4, 2, 3, 5)
    return out.reshape(1, count, EZ, EY, PTS)


def solution(mesh):
    return jax.shard_map(
        body,
        mesh=mesh,
        in_specs=(
            P("layer", "slab", None, None, None),
            P("layer", "slab", None, None, None, None),
            P(),
            P("slab", None),
        ),
        out_specs=P("layer", "slab", None, None, None),
        check_vma=False,
    )
```

```python
import functools

import jax
import jax.numpy as jnp
import numpy as np
from jax import lax
from jax.experimental import pallas as pl
from jax.experimental.pallas import tpu as pltpu
from jax.sharding import PartitionSpec as P

P_SIZE = 8
PTS = 512
EY = 4
EZ = 4
CHUNK = 8
AHEAD = 3
HOLD = 3
FACES, EDGES, BOTH = (0, 1, 2), (3, 4), (0, 1, 2, 3, 4)
LAST = 16
GATHER = 32
F32 = jnp.float32
BF16 = jnp.bfloat16
MESH = pl.DeviceIdType.MESH


def legendre_pair(gll_nodes, degree):
    lower_poly = gll_nodes * 0.0 + 1.0
    upper_poly = gll_nodes.copy()
    for poly_order in range(2, degree + 1):
        lower_poly, upper_poly = (
            upper_poly,
            ((2 * poly_order - 1) * gll_nodes * upper_poly - (poly_order - 1) * lower_poly)
            / poly_order,
        )
    return (lower_poly, upper_poly)


def gll_tables():
    degree = P_SIZE - 1
    gll_nodes = -np.cos(np.pi * np.arange(P_SIZE) / degree)
    for newton_sweep in range(100):
        lower_poly, upper_poly = legendre_pair(gll_nodes, degree)
        gll_nodes = gll_nodes - (gll_nodes * upper_poly - lower_poly) / ((degree + 1) * upper_poly)
    lower_poly, upper_poly = legendre_pair(gll_nodes, degree)
    quad_weights = 2.0 / (degree * (degree + 1) * upper_poly * upper_poly)
    identity = np.eye(P_SIZE)
    differ = gll_nodes[:, None] - gll_nodes[None, :] + identity
    derivative = upper_poly[:, None] / (upper_poly[None, :] * differ)
    derivative = derivative * (1.0 - identity)
    derivative[0, 0] = -degree * (degree + 1) / 4.0
    derivative[degree, degree] = degree * (degree + 1) / 4.0
    return derivative, quad_weights


def parts(table):
    high = np.asarray(table, np.float32).astype(BF16)
    low = (table - high.astype(np.float64)).astype(np.float32).astype(BF16)
    return high, low


def constant_tables():
    derivative, rho = gll_tables()
    eye = np.eye(P_SIZE)
    pair = np.eye(2)
    x_in = np.kron(pair, np.kron(eye, derivative.T))
    y_in = np.kron(pair, np.kron(derivative.T, eye))
    x_out = np.kron(pair, np.kron(eye, derivative))
    y_out = np.kron(pair, np.kron(derivative, eye))
    high, low = parts(np.concatenate([x_in, y_in], 1))
    matrices = [high, low]
    for table in (x_out, y_out):
        matrices.append(np.concatenate(parts(table), 1))
    sub = np.arange(8)[:, None] // 4
    lane = np.arange(128)[None, :]
    c_low = 2 * sub + lane // 64
    vectors = []
    for table in (derivative, derivative.T):
        for half in range(2):
            for source in range(2):
                for move in (0, 2, 1, 3):
                    vectors.append(table[4 * half + c_low, 4 * source + (c_low ^ move)])
    plane = rho[lane // 8 % 8] * rho[lane % 8]
    for half in range(2):
        vectors.append(rho[4 * half + c_low] * plane)
    return np.stack(matrices), np.stack(vectors).astype(np.float32)


def turn(value, shift):
    return pltpu.roll(value, shift % 128, axis=value.ndim - 1) if shift % 128 else value


def spin(value, shift):
    return pltpu.roll(value, (shift + 256) & 127, axis=1)


def slide(value, shift):
    return pltpu.roll(value, shift % 8, axis=value.ndim - 2)


def mirror(value):
    return slide(turn(value, 64), 4)


def iotas():
    sub = lax.broadcasted_iota(jnp.int32, (8, 128), 0)
    lane = lax.broadcasted_iota(jnp.int32, (8, 128), 1)
    return sub, lane


def split(value):
    high = value.astype(BF16)
    low = (value - high.astype(F32)).astype(BF16)
    return jnp.concatenate([high, low], axis=-1)


def product(both, matrix):
    return jnp.dot(both, jnp.concatenate([matrix, matrix], 0), preferred_element_type=F32)


def along_z(low, high, low_turned, high_turned, table_ref, start):
    terms = []
    for value, turned in ((low, low_turned), (high, high_turned)):
        terms += [value, slide(value, 4), turned, slide(turned, 4)]
    out = []
    for half in range(2):
        total = table_ref[start + 8 * half] * terms[0]
        for k in range(1, 8):
            total += table_ref[start + 8 * half + k] * terms[k]
        out.append(total)
    return out


def flip_faces(value, sub, lane, shift):
    value = jnp.take_along_axis(value, sub ^ 3, axis=0)
    return jnp.take_along_axis(value, ((((lane - shift) & 127) ^ 56) + shift) & 127, axis=1)


def edge_mask(sub, lane, slot):
    base = jnp.where(sub < 4, 0, 71)
    return ((lane - base - slot) & 71) == 0


def chunk_fluxes(u_ref, m_ref, mat_ref, vec_ref, fx_ref, fy_ref, fz_ref):
    count = u_ref.shape[0]
    rows = count * EZ * 2 * 8
    u = u_ref[...].reshape(rows, 128)
    both = split(u)
    grads = product(both, mat_ref[0]) + product(both, mat_ref[1])
    weights = [vec_ref[32], vec_ref[33]]
    turned = turn(u, 64)
    flux_x, flux_y = [], []
    for s in range(count):
        for ez in range(EZ):
            at = (s * EZ + ez) * 16
            pieces = along_z(
                u[at : at + 8], u[at + 8 : at + 16], turned[at : at + 8], turned[at + 8 : at + 16], vec_ref, 0
            )
            for h in range(2):
                grad = grads[at + 8 * h : at + 8 * h + 8]
                fz_ref[at // 8 + h] = pieces[h] * (weights[h] * m_ref[s, ez, 2, h])
                flux_x.append(grad[:, :128] * (weights[h] * m_ref[s, ez, 0, h]))
                flux_y.append(grad[:, 128:] * (weights[h] * m_ref[s, ez, 1, h]))
    fx_ref[...] = split(jnp.concatenate(flux_x, 0))
    fy_ref[...] = split(jnp.concatenate(flux_y, 0))


def chunk_local(fx_ref, fy_ref, fz_ref, mat_ref, vec_ref, flip_mask, sub, lane, offset):
    count = CHUNK
    result = product(fx_ref[...], mat_ref[2]) + product(fy_ref[...], mat_ref[3])
    flux_z = [fz_ref[k] for k in range(2 * count * EZ)]
    flux_turned = [turn(value, 64) for value in flux_z]
    out_z = [
        along_z(flux_z[k], flux_z[k + 1], flux_turned[k], flux_turned[k + 1], vec_ref, 16)
        for k in range(0, 2 * count * EZ, 2)
    ]
    b = (lane >> 3) & 7
    a = lane & 7
    ey = sub & 3
    swap = jnp.where((b == 0) | (b == 7), lane ^ 56, lane)
    high_b = (b == 7) & (ey < 3)
    low_b = (b == 0) & (ey > 0)
    bottom = (sub < 4) & (lane < 64)
    top = (sub >= 4) & (lane >= 64)
    diagonal = bottom | top
    local, lefts, rights, z_own = [], [], [], []
    for s in range(count):
        block = []
        for ez in range(EZ):
            for h in range(2):
                at = (s * EZ + ez) * 16 + 8 * h
                v = result[at : at + 8, :128] + result[at : at + 8, 128:] + out_z[s * EZ + ez][h]
                swapped = jnp.take_along_axis(v, swap, axis=1)
                met = jnp.where(high_b, slide(swapped, -1), jnp.where(low_b, slide(swapped, 1), 0.0))
                block.append(v + met)
        for ez in range(EZ - 1):
            upper, lower = block[2 * ez + 1], block[2 * ez + 2]
            block[2 * ez + 2] = jnp.where(bottom, lower + mirror(upper), lower)
            block[2 * ez + 1] = jnp.where(top, upper + mirror(lower), upper)
        left = right = block[0]
        for j in range(1, 8):
            moved = turn(block[j], j)
            left = jnp.where(a == j, moved, left)
            right = jnp.where(a == j - 1, moved, right)
        right = jnp.where(flip_mask(s), flip_faces(right, sub, lane, 7), right)
        local.append(block)
        lefts.append(left)
        rights.append(right)
        z_own.append(jnp.where(bottom, block[0], block[7]))
    z_pairs = [
        jnp.where(diagonal, z_own[s], turn(z_own[s + 1], 64)) for s in range(0, count, 2)
    ]
    edges = []
    for faces, shift in ((lefts, 0), (rights, 7)):
        packed = faces[0]
        for s in range(1, count):
            packed = jnp.where(edge_mask(sub, lane, s + shift), turn(faces[s], s), packed)
        moved = slide(packed, 4)
        edges.append(jnp.where(sub < 4, spin(moved, offset - 71 - shift), spin(moved, offset + 71 - shift)))
    return local, lefts, rights, z_pairs, edges


def positions(wanted, values, offset, count):
    t = lax.broadcasted_iota(jnp.int32, (count, 128), 0)
    lane = lax.broadcasted_iota(jnp.int32, (count, 128), 1)
    column = jnp.sum(jnp.where(lane == t + offset, values, 0).astype(F32), axis=1, keepdims=True)
    hit = column == wanted.astype(F32)
    return jnp.sum(jnp.where(hit, t, 0).astype(F32), axis=0, keepdims=True).astype(jnp.int32)


def main_kernel(
    u_hbm, m_hbm, mat_hbm, vec_hbm, fm_hbm, ids_hbm,
    local, left_in, right_in, z_in, el_in, er_in, fm, pos,
    u_v, m_v, fx, fy, fz, mat, vec, ids, pos_v, left, right, z, el, er,
    in_sem, one_sem, send_sem, recv_sem,
):
    cycle = lax.axis_size("slab")
    me = lax.axis_index("slab")
    layer = lax.axis_index("layer")
    after, before = lax.rem(me + 1, cycle), lax.rem(me + cycle - 1, cycle)
    other = 1 - layer
    peers = [(after, layer), (before, layer), (me, other), (after, other), (before, other)]
    count = local.shape[0]
    steps = count // CHUNK
    total = cycle * count
    barrier = pltpu.get_barrier_semaphore()
    for s, l in peers:
        pl.semaphore_signal(barrier, inc=1, device_id={"slab": s, "layer": l}, device_id_type=MESH)

    def loads(i):
        part = pl.ds(i * CHUNK, CHUNK)
        return [
            pltpu.make_async_copy(u_hbm.at[part], u_v.at[part], in_sem.at[0, i]),
            pltpu.make_async_copy(m_hbm.at[part], m_v.at[part], in_sem.at[1, i]),
        ]

    def once():
        pairs = [(mat_hbm, mat), (vec_hbm, vec), (fm_hbm.at[:, pl.ds(0, 128)], fm), (ids_hbm, ids)]
        return [pltpu.make_async_copy(a, b, one_sem.at[k]) for k, (a, b) in enumerate(pairs)]

    for copy in loads(0) + once():
        copy.start()
    for i in range(1, AHEAD):
        for copy in loads(i):
            copy.start()
    for copy in once():
        copy.wait()

    per_row = 128 // count
    rows = [ids[pl.ds(d // per_row, 1), :] for d in (me, before, after)]
    sub, lane = iotas()
    found = []
    for row, device, move in ((rows[1], before, total - 1), (rows[2], after, 1)):
        wanted = rows[0] + move
        wanted = jnp.where(wanted >= total, wanted - total, wanted)
        found.append(positions(wanted, row, lax.rem(device, per_row) * count, count))
    pos_v[...] = jnp.where(sub == 0, found[0], found[1])
    pos_copy = pltpu.make_async_copy(pos_v, pos, one_sem.at[4])
    pos_copy.start()

    def sends(i, chunks, kinds):
        part = pl.ds(i * CHUNK, chunks * CHUNK)
        half = pl.ds(i * (CHUNK // 2), chunks * (CHUNK // 2))
        single = pl.ds(i // 2, chunks // 2)
        jobs = [(right, right_in, part), (left, left_in, part), (z, z_in, half), (er, er_in, single), (el, el_in, single)]
        return [
            pltpu.make_async_remote_copy(
                src_ref=src.at[at],
                dst_ref=dst.at[at],
                send_sem=send_sem.at[k],
                recv_sem=recv_sem.at[k],
                device_id={"slab": s, "layer": l},
                device_id_type=MESH,
            )
            for k, ((src, dst, at), (s, l)) in enumerate(zip(jobs, peers))
            if k in kinds
        ]

    def fluxes(i):
        for copy in loads(i):
            copy.wait()
        part = pl.ds(i * CHUNK, CHUNK)
        chunk_fluxes(u_v.at[part], m_v.at[part], mat, vec, fx, fy, fz)

    def assemble(i):
        def flip_mask(s):
            return fm[pl.ds(i * CHUNK + s, 1), :] != lane

        blocks, lefts, rights, z_pairs, edges = chunk_local(
            fx, fy, fz, mat, vec, flip_mask, sub, lane, lax.rem(i, 2) * 64
        )
        for s in range(CHUNK):
            for j in range(8):
                local[i * CHUNK + s, j // 2, j % 2] = blocks[s][j]
            left[i * CHUNK + s] = lefts[s]
            right[i * CHUNK + s] = rights[s]
        for s in range(CHUNK // 2):
            z[i * (CHUNK // 2) + s] = z_pairs[s]
        first_of_two = jnp.where(sub < 4, lane, (lane - 71) & 127) < 64
        odd = lax.rem(i, 2) == 1
        for ref, edge in ((el, edges[0]), (er, edges[1])):
            held = ref[i // 2]
            ref[i // 2] = jnp.where(odd, jnp.where(first_of_two, held, edge), edge)

    def launch(i):
        @pl.when(i == HOLD)
        def _():
            pl.semaphore_wait(barrier, 5)
            for copy in sends(0, HOLD + 1, BOTH):
                copy.start()

        @pl.when((i > HOLD) & (lax.rem(i, 2) == 0))
        def _():
            for copy in sends(i, 1, FACES):
                copy.start()

        @pl.when((i > HOLD) & (lax.rem(i, 2) == 1))
        def _():
            for copy in sends(i, 1, FACES) + sends(i - 1, 2, EDGES):
                copy.start()

    fluxes(0)

    def step(i, carry):
        for copy in loads(i):
            copy.wait()

        @pl.when(i + AHEAD - 1 < steps)
        def _():
            for copy in loads(i + AHEAD - 1):
                copy.start()

        assemble(i - 1)
        part = pl.ds(i * CHUNK, CHUNK)
        chunk_fluxes(u_v.at[part], m_v.at[part], mat, vec, fx, fy, fz)
        launch(i - 1)
        return carry

    lax.fori_loop(1, steps, step, 0)
    assemble(steps - 1)
    for copy in sends(steps - 1, 1, FACES) + sends(steps - 2, 2, EDGES):
        copy.start()
    pos_copy.wait()
    for copy in sends(0, steps, BOTH):
        copy.wait()


def final_kernel(local, left_in, right_in, z_in, el_in, er_in, fm, pos, out_hbm, out, faces, sem):
    sub, lane = iotas()
    count = local.shape[0]
    per_row = 128 // count
    first = lax.rem(lax.axis_index("slab"), per_row) * count
    on_edge = edge_mask(sub, lane, 0)
    even = (lane & 1) == 0
    a = lane & 7
    on_face = (a == 0) | (a == 7)
    bottom = (sub < 4) & (lane < 64)
    top = (sub >= 4) & (lane >= 64)

    def write(i):
        part = pl.ds(i * LAST, LAST)
        return pltpu.make_async_copy(out.at[part], out_hbm.at[part], sem.at[i])

    def edge(edge_ref, at):
        slot = ((at & 8) << 3) | (at & 7)
        return jnp.where(on_edge, pltpu.roll(edge_ref[at >> 4], (128 - slot) & 127, axis=1), 0.0)

    def gather(i, carry):
        for s in range(GATHER):
            slab = i * GATHER + s
            back, ahead = pos[0, first + slab], pos[1, first + slab]
            low = turn(right_in[back], -7) + edge(er_in, back)
            high = left_in[ahead] + edge(el_in, ahead)
            flipped = fm[pl.ds(slab, 1), :] != lane
            high = turn(jnp.where(flipped, flip_faces(high, sub, lane, 0), high), 7)
            faces[slab, 0] = jnp.where(even, low, high)
            faces[slab, 1] = jnp.where(even, high, low)
        return carry

    lax.fori_loop(0, count // GATHER, gather, 0)

    def step(i, carry):
        for s in range(LAST):
            slab = i * LAST + s
            z = slide(z_in[i * (LAST // 2) + s // 2], 4)
            z = z if s % 2 else turn(z, 64)
            for j in range(8):
                v = local[slab, j // 2, j % 2] + jnp.where(on_face, turn(faces[slab, j % 2], -j), 0.0)
                if j == 0:
                    v += jnp.where(bottom, z, 0.0)
                if j == 7:
                    v += jnp.where(top, z, 0.0)
                out[slab, j // 2, j % 2] = v
        write(i).start()
        return carry

    lax.fori_loop(0, count // LAST, step, 0)

    def finish(i, carry):
        write(i).wait()
        return carry

    lax.fori_loop(0, count // LAST, finish, 0)


def body(nodal_field, metric, slab_ids, face_map):
    count = nodal_field.shape[1]
    steps = count // CHUNK
    u = nodal_field.reshape(count, EZ, EY, 2, 2, 128).transpose(0, 1, 3, 4, 2, 5)
    u = u.reshape(count, EZ, 2, 8, 128)
    m = metric.reshape(count, EZ, EY, 3, 2, 2, 128).transpose(0, 1, 3, 4, 5, 2, 6)
    m = m.reshape(count, EZ, 3, 2, 8, 128)
    ids = slab_ids.reshape(-1, 128)
    matrices, vectors = constant_tables()
    matrices, vectors = jnp.asarray(matrices), jnp.asarray(vectors)
    hbm = pl.BlockSpec(memory_space=pltpu.HBM)
    vmem = pl.BlockSpec(memory_space=pltpu.VMEM)
    smem = pl.BlockSpec(memory_space=pltpu.SMEM)
    whole = (count, EZ, 2, 8, 128)
    face, z_face, edge = (count, 8, 128), (count // 2, 8, 128), (steps // 2, 8, 128)
    dma = pltpu.SemaphoreType.DMA
    shared = pl.pallas_call(
        main_kernel,
        in_specs=[hbm] * 6,
        out_specs=[vmem] * 7 + [smem],
        out_shape=[pltpu.VMEM(s, F32) for s in (whole, face, face, z_face, edge, edge)]
        + [pltpu.VMEM((count, 128), jnp.int32), pltpu.SMEM((8, 128), jnp.int32)],
        scratch_shapes=[
            pltpu.VMEM(u.shape, F32),
            pltpu.VMEM(m.shape, F32),
            pltpu.VMEM((CHUNK * EZ * 16, 256), BF16),
            pltpu.VMEM((CHUNK * EZ * 16, 256), BF16),
            pltpu.VMEM((CHUNK * EZ * 2, 8, 128), F32),
            pltpu.VMEM(matrices.shape, BF16),
            pltpu.VMEM(vectors.shape, F32),
            pltpu.VMEM(ids.shape, jnp.int32),
            pltpu.VMEM((8, 128), jnp.int32),
            pltpu.VMEM(face, F32),
            pltpu.VMEM(face, F32),
            pltpu.VMEM(z_face, F32),
            pltpu.VMEM(edge, F32),
            pltpu.VMEM(edge, F32),
            dma((2, steps)),
            dma((5,)),
            dma((5,)),
            dma((5,)),
        ],
        compiler_params=pltpu.CompilerParams(
            collective_id=0, has_side_effects=True, vmem_limit_bytes=60 * 2**20
        ),
    )(u, m, matrices, vectors, face_map, ids)
    out = pl.pallas_call(
        final_kernel,
        in_specs=[vmem] * 7 + [smem],
        out_specs=hbm,
        out_shape=jax.ShapeDtypeStruct(whole, F32),
        scratch_shapes=[pltpu.VMEM(whole, F32), pltpu.VMEM((count, 2, 8, 128), F32), dma((count // LAST,))],
        compiler_params=pltpu.CompilerParams(vmem_limit_bytes=40 * 2**20),
    )(*shared)
    out = out.reshape(count, EZ, 2, 2, EY, 128).transpose(0, 1, 4, 2, 3, 5)
    return out.reshape(1, count, EZ, EY, PTS)


def solution(mesh):
    return jax.shard_map(
        body,
        mesh=mesh,
        in_specs=(
            P("layer", "slab", None, None, None),
            P("layer", "slab", None, None, None, None),
            P(),
            P("slab", None),
        ),
        out_specs=P("layer", "slab", None, None, None),
        check_vma=False,
    )
```

```python
import functools

import jax
import jax.numpy as jnp
import numpy as np
from jax import lax
from jax.experimental import pallas as pl
from jax.experimental.pallas import tpu as pltpu
from jax.sharding import PartitionSpec as P

P_SIZE = 8
PTS = 512
EY = 4
EZ = 4
CHUNK = 8
AHEAD = 3
HOLD = 3
FACES, EDGES, BOTH = (0, 1, 2), (3, 4), (0, 1, 2, 3, 4)
LAST = 16
GATHER = 32
F32 = jnp.float32
BF16 = jnp.bfloat16
MESH = pl.DeviceIdType.MESH


def legendre_pair(gll_nodes, degree):
    lower_poly = gll_nodes * 0.0 + 1.0
    upper_poly = gll_nodes.copy()
    for poly_order in range(2, degree + 1):
        lower_poly, upper_poly = (
            upper_poly,
            ((2 * poly_order - 1) * gll_nodes * upper_poly - (poly_order - 1) * lower_poly)
            / poly_order,
        )
    return (lower_poly, upper_poly)


def gll_tables():
    degree = P_SIZE - 1
    gll_nodes = -np.cos(np.pi * np.arange(P_SIZE) / degree)
    for newton_sweep in range(100):
        lower_poly, upper_poly = legendre_pair(gll_nodes, degree)
        gll_nodes = gll_nodes - (gll_nodes * upper_poly - lower_poly) / ((degree + 1) * upper_poly)
    lower_poly, upper_poly = legendre_pair(gll_nodes, degree)
    quad_weights = 2.0 / (degree * (degree + 1) * upper_poly * upper_poly)
    identity = np.eye(P_SIZE)
    differ = gll_nodes[:, None] - gll_nodes[None, :] + identity
    derivative = upper_poly[:, None] / (upper_poly[None, :] * differ)
    derivative = derivative * (1.0 - identity)
    derivative[0, 0] = -degree * (degree + 1) / 4.0
    derivative[degree, degree] = degree * (degree + 1) / 4.0
    return derivative, quad_weights


def parts(table):
    high = np.asarray(table, np.float32).astype(BF16)
    low = (table - high.astype(np.float64)).astype(np.float32).astype(BF16)
    return high, low


def constant_tables():
    derivative, rho = gll_tables()
    eye = np.eye(P_SIZE)
    pair = np.eye(2)
    x_in = np.kron(pair, np.kron(eye, derivative.T))
    y_in = np.kron(pair, np.kron(derivative.T, eye))
    x_out = np.kron(pair, np.kron(eye, derivative))
    y_out = np.kron(pair, np.kron(derivative, eye))
    lane = np.arange(128)[None, :]
    plane = rho[lane // 8 % 8] * rho[lane % 8]
    high, low = parts(np.concatenate([x_in * plane, y_in * plane], 1))
    matrices = [high, low]
    for table in (x_out, y_out):
        matrices.append(np.concatenate(parts(table), 1))
    sub = np.arange(8)[:, None] // 4
    c_low = 2 * sub + lane // 64
    vectors = []
    for table, weight in ((derivative, rho[c_low] * plane), (derivative.T, 1.0)):
        for sign in (1.0, -1.0):
            for move in (0, 1, 2, 3):
                other = c_low ^ move
                term = weight * (table[c_low, other] + sign * table[c_low, 7 - other]) / 2
                vectors.append(np.roll(term, 4, 0) if move > 1 else term)
    for half in range(2):
        vectors.append(rho[4 * half + c_low] + 0.0 * plane)
    return np.stack(matrices), np.stack(vectors).astype(np.float32)


def turn(value, shift):
    return pltpu.roll(value, shift % 128, axis=value.ndim - 1) if shift % 128 else value


def spin(value, shift):
    return pltpu.roll(value, (shift + 256) & 127, axis=1)


def slide(value, shift):
    return pltpu.roll(value, shift % 8, axis=value.ndim - 2)


def mirror(value):
    return slide(turn(value, 64), 4)


def iotas():
    sub = lax.broadcasted_iota(jnp.int32, (8, 128), 0)
    lane = lax.broadcasted_iota(jnp.int32, (8, 128), 1)
    return sub, lane


def split(value):
    high = value.astype(BF16)
    low = (value - high.astype(F32)).astype(BF16)
    return jnp.concatenate([high, low], axis=-1)


def product(both, matrix):
    return jnp.dot(both, jnp.concatenate([matrix, matrix], 0), preferred_element_type=F32)


def along_z(low, high, low_turned, high_turned, table_ref, start):
    back, back_turned = slide(high_turned, 4), slide(high, 4)
    halves = []
    for value, turned, first in (
        (low + back, low_turned + back_turned, start),
        (low - back, low_turned - back_turned, start + 4),
    ):
        near = table_ref[first] * value + table_ref[first + 1] * turned
        far = table_ref[first + 2] * value + table_ref[first + 3] * turned
        halves.append(near + slide(far, 4))
    even, odd = halves
    return even + odd, mirror(odd - even)


def flip_faces(value, sub, lane, shift):
    value = jnp.take_along_axis(value, sub ^ 3, axis=0)
    return jnp.take_along_axis(value, ((((lane - shift) & 127) ^ 56) + shift) & 127, axis=1)


def edge_mask(sub, lane, slot):
    base = jnp.where(sub < 4, 0, 71)
    return ((lane - base - slot) & 71) == 0


def chunk_fluxes(u_ref, m_ref, mat_ref, vec_ref, fx_ref, fy_ref, fz_ref):
    count = u_ref.shape[0]
    rows = count * EZ * 2 * 8
    u = u_ref[...].reshape(rows, 128)
    scaled = u.reshape(count * EZ, 2, 8, 128) * vec_ref[16:18]
    both = split(scaled.reshape(rows, 128))
    grads = product(both, mat_ref[0]) + product(both, mat_ref[1])
    turned = turn(u, 64)
    flux_x, flux_y = [], []
    for s in range(count):
        for ez in range(EZ):
            at = (s * EZ + ez) * 16
            pieces = along_z(
                u[at : at + 8], u[at + 8 : at + 16], turned[at : at + 8], turned[at + 8 : at + 16], vec_ref, 0
            )
            for h in range(2):
                grad = grads[at + 8 * h : at + 8 * h + 8]
                fz_ref[at // 8 + h] = pieces[h] * m_ref[s, ez, 2, h]
                flux_x.append(grad[:, :128] * m_ref[s, ez, 0, h])
                flux_y.append(grad[:, 128:] * m_ref[s, ez, 1, h])
    fx_ref[...] = split(jnp.concatenate(flux_x, 0))
    fy_ref[...] = split(jnp.concatenate(flux_y, 0))


def corners(sub, lane):
    return (sub < 4) & (lane < 64), (sub >= 4) & (lane >= 64)


def chunk_local(fx_ref, fy_ref, fz_ref, mat_ref, vec_ref, sub, lane, put):
    count = CHUNK
    result = product(fx_ref[...], mat_ref[2]) + product(fy_ref[...], mat_ref[3])
    flux_z = [fz_ref[k] for k in range(2 * count * EZ)]
    flux_turned = [turn(value, 64) for value in flux_z]
    out_z = [
        along_z(flux_z[k], flux_z[k + 1], flux_turned[k], flux_turned[k + 1], vec_ref, 8)
        for k in range(0, 2 * count * EZ, 2)
    ]
    b = (lane >> 3) & 7
    ey = sub & 3
    swap = jnp.where((b == 0) | (b == 7), lane ^ 56, lane)
    high_b = (b == 7) & (ey < 3)
    low_b = (b == 0) & (ey > 0)
    bottom, top = corners(sub, lane)
    for s in range(count):
        block = []
        for ez in range(EZ):
            for h in range(2):
                at = (s * EZ + ez) * 16 + 8 * h
                v = result[at : at + 8, :128] + result[at : at + 8, 128:] + out_z[s * EZ + ez][h]
                swapped = jnp.take_along_axis(v, swap, axis=1)
                met = jnp.where(high_b, slide(swapped, -1), jnp.where(low_b, slide(swapped, 1), 0.0))
                block.append(v + met)
        for ez in range(EZ - 1):
            upper, lower = block[2 * ez + 1], block[2 * ez + 2]
            block[2 * ez + 2] = jnp.where(bottom, lower + mirror(upper), lower)
            block[2 * ez + 1] = jnp.where(top, upper + mirror(lower), upper)
        for j in range(8):
            put(s, j, block[j])


def chunk_pack(stage_ref, flip_mask, sub, lane, offset):
    count = CHUNK
    a = lane & 7
    bottom, top = corners(sub, lane)
    lefts, rights, z_own = [], [], []
    for s in range(count):
        left = right = stage_ref[s, 0]
        for j in range(1, 8):
            moved = turn(stage_ref[s, j], j)
            left = jnp.where(a == j, moved, left)
            right = jnp.where(a == j - 1, moved, right)
        right = jnp.where(flip_mask(s), flip_faces(right, sub, lane, 7), right)
        lefts.append(left)
        rights.append(right)
        z_own.append(jnp.where(bottom, stage_ref[s, 0], stage_ref[s, 7]))
    z_pairs = [
        jnp.where(bottom | top, z_own[s], turn(z_own[s + 1], 64)) for s in range(0, count, 2)
    ]
    edges = []
    for faces, shift in ((lefts, 0), (rights, 7)):
        packed = faces[0]
        for s in range(1, count):
            packed = jnp.where(edge_mask(sub, lane, s + shift), turn(faces[s], s), packed)
        moved = slide(packed, 4)
        edges.append(jnp.where(sub < 4, spin(moved, offset - 71 - shift), spin(moved, offset + 71 - shift)))
    return lefts, rights, z_pairs, edges


def positions(wanted, values, offset, count):
    t = lax.broadcasted_iota(jnp.int32, (count, 128), 0)
    lane = lax.broadcasted_iota(jnp.int32, (count, 128), 1)
    column = jnp.sum(jnp.where(lane == t + offset, values, 0).astype(F32), axis=1, keepdims=True)
    hit = column == wanted.astype(F32)
    return jnp.sum(jnp.where(hit, t, 0).astype(F32), axis=0, keepdims=True).astype(jnp.int32)


def main_kernel(
    u_hbm, m_hbm, mat_hbm, vec_hbm, fm_hbm, ids_hbm,
    local, left_in, right_in, z_in, el_in, er_in, fm, pos,
    u_v, m_v, fx, fy, fz, stage, mat, vec, ids, pos_v, left, right, z, el, er,
    in_sem, one_sem, send_sem, recv_sem,
):
    cycle = lax.axis_size("slab")
    me = lax.axis_index("slab")
    layer = lax.axis_index("layer")
    after, before = lax.rem(me + 1, cycle), lax.rem(me + cycle - 1, cycle)
    other = 1 - layer
    peers = [(after, layer), (before, layer), (me, other), (after, other), (before, other)]
    count = local.shape[0]
    steps = count // CHUNK
    total = cycle * count
    barrier = pltpu.get_barrier_semaphore()
    for s, l in peers:
        pl.semaphore_signal(barrier, inc=1, device_id={"slab": s, "layer": l}, device_id_type=MESH)

    def loads(i):
        part = pl.ds(i * CHUNK, CHUNK)
        return [
            pltpu.make_async_copy(u_hbm.at[part], u_v.at[part], in_sem.at[0, i]),
            pltpu.make_async_copy(m_hbm.at[part], m_v.at[part], in_sem.at[1, i]),
        ]

    def once():
        pairs = [(mat_hbm, mat), (vec_hbm, vec), (fm_hbm.at[:, pl.ds(0, 128)], fm), (ids_hbm, ids)]
        return [pltpu.make_async_copy(a, b, one_sem.at[k]) for k, (a, b) in enumerate(pairs)]

    for copy in loads(0) + once():
        copy.start()
    for i in range(1, AHEAD - 1):
        for copy in loads(i):
            copy.start()
    for copy in once():
        copy.wait()

    per_row = 128 // count
    rows = [ids[pl.ds(d // per_row, 1), :] for d in (me, before, after)]
    sub, lane = iotas()
    found = []
    for row, device, move in ((rows[1], before, total - 1), (rows[2], after, 1)):
        wanted = rows[0] + move
        wanted = jnp.where(wanted >= total, wanted - total, wanted)
        found.append(positions(wanted, row, lax.rem(device, per_row) * count, count))
    pos_v[...] = jnp.where(sub == 0, found[0], found[1])
    pos_copy = pltpu.make_async_copy(pos_v, pos, one_sem.at[4])
    pos_copy.start()

    def sends(i, chunks, kinds):
        part = pl.ds(i * CHUNK, chunks * CHUNK)
        half = pl.ds(i * (CHUNK // 2), chunks * (CHUNK // 2))
        single = pl.ds(i // 2, chunks // 2)
        jobs = [(right, right_in, part), (left, left_in, part), (z, z_in, half), (er, er_in, single), (el, el_in, single)]
        return [
            pltpu.make_async_remote_copy(
                src_ref=src.at[at],
                dst_ref=dst.at[at],
                send_sem=send_sem.at[k],
                recv_sem=recv_sem.at[k],
                device_id={"slab": s, "layer": l},
                device_id_type=MESH,
            )
            for k, ((src, dst, at), (s, l)) in enumerate(zip(jobs, peers))
            if k in kinds
        ]

    def fluxes(i):
        part = pl.ds(i * CHUNK, CHUNK)
        chunk_fluxes(u_v.at[part], m_v.at[part], mat, vec, fx, fy, fz)

    def assemble(i):
        def put(s, j, value):
            local[i * CHUNK + s, j // 2, j % 2] = value
            stage[s, j] = value

        chunk_local(fx, fy, fz, mat, vec, sub, lane, put)

    def pack(i):
        def flip_mask(s):
            return fm[pl.ds(i * CHUNK + s, 1), :] != lane

        lefts, rights, z_pairs, edges = chunk_pack(stage, flip_mask, sub, lane, lax.rem(i, 2) * 64)
        for s in range(CHUNK):
            left[i * CHUNK + s] = lefts[s]
            right[i * CHUNK + s] = rights[s]
        for s in range(CHUNK // 2):
            z[i * (CHUNK // 2) + s] = z_pairs[s]
        first_of_two = jnp.where(sub < 4, lane, (lane - 71) & 127) < 64
        odd = lax.rem(i, 2) == 1
        for ref, edge in ((el, edges[0]), (er, edges[1])):
            held = ref[i // 2]
            ref[i // 2] = jnp.where(odd, jnp.where(first_of_two, held, edge), edge)

    def arrive(i):
        for copy in loads(i):
            copy.wait()

        @pl.when(i + AHEAD - 1 < steps)
        def _():
            for copy in loads(i + AHEAD - 1):
                copy.start()

    def launch(i):
        @pl.when(i == HOLD)
        def _():
            pl.semaphore_wait(barrier, 5)
            for copy in sends(0, HOLD + 1, BOTH):
                copy.start()

        @pl.when((i > HOLD) & (lax.rem(i, 2) == 0))
        def _():
            for copy in sends(i, 1, FACES):
                copy.start()

        @pl.when((i > HOLD) & (lax.rem(i, 2) == 1))
        def _():
            for copy in sends(i, 1, FACES) + sends(i - 1, 2, EDGES):
                copy.start()

    arrive(0)
    fluxes(0)
    arrive(1)
    assemble(0)
    fluxes(1)

    def step(i, carry):
        arrive(i)
        pack(i - 2)
        assemble(i - 1)
        fluxes(i)
        launch(i - 2)
        return carry

    lax.fori_loop(2, steps, step, 0)
    pack(steps - 2)
    assemble(steps - 1)
    for copy in sends(steps - 2, 1, FACES):
        copy.start()
    pack(steps - 1)
    for copy in sends(steps - 1, 1, FACES) + sends(steps - 2, 2, EDGES):
        copy.start()
    pos_copy.wait()
    for copy in sends(0, steps, BOTH):
        copy.wait()


def final_kernel(local, left_in, right_in, z_in, el_in, er_in, fm, pos, out_hbm, out, faces, sem):
    sub, lane = iotas()
    count = local.shape[0]
    per_row = 128 // count
    first = lax.rem(lax.axis_index("slab"), per_row) * count
    on_edge = edge_mask(sub, lane, 0)
    even = (lane & 1) == 0
    a = lane & 7
    on_face = (a == 0) | (a == 7)
    bottom = (sub < 4) & (lane < 64)
    top = (sub >= 4) & (lane >= 64)

    def write(i):
        part = pl.ds(i * LAST, LAST)
        return pltpu.make_async_copy(out.at[part], out_hbm.at[part], sem.at[i])

    def edge(edge_ref, at):
        slot = ((at & 8) << 3) | (at & 7)
        return jnp.where(on_edge, pltpu.roll(edge_ref[at >> 4], (128 - slot) & 127, axis=1), 0.0)

    def gather(i, carry):
        for s in range(GATHER):
            slab = i * GATHER + s
            back, ahead = pos[0, first + slab], pos[1, first + slab]
            low = turn(right_in[back], -7) + edge(er_in, back)
            high = left_in[ahead] + edge(el_in, ahead)
            flipped = fm[pl.ds(slab, 1), :] != lane
            high = turn(jnp.where(flipped, flip_faces(high, sub, lane, 0), high), 7)
            faces[slab, 0] = jnp.where(even, low, high)
            faces[slab, 1] = jnp.where(even, high, low)
        return carry

    lax.fori_loop(0, count // GATHER, gather, 0)

    def step(i, carry):
        for s in range(LAST):
            slab = i * LAST + s
            z = slide(z_in[i * (LAST // 2) + s // 2], 4)
            z = z if s % 2 else turn(z, 64)
            for j in range(8):
                v = local[slab, j // 2, j % 2] + jnp.where(on_face, turn(faces[slab, j % 2], -j), 0.0)
                if j == 0:
                    v += jnp.where(bottom, z, 0.0)
                if j == 7:
                    v += jnp.where(top, z, 0.0)
                out[slab, j // 2, j % 2] = v
        write(i).start()
        return carry

    lax.fori_loop(0, count // LAST, step, 0)

    def finish(i, carry):
        write(i).wait()
        return carry

    lax.fori_loop(0, count // LAST, finish, 0)


def body(nodal_field, metric, slab_ids, face_map):
    count = nodal_field.shape[1]
    steps = count // CHUNK
    u = nodal_field.reshape(count, EZ, EY, 2, 2, 128).transpose(0, 1, 3, 4, 2, 5)
    u = u.reshape(count, EZ, 2, 8, 128)
    m = metric.reshape(count, EZ, EY, 3, 2, 2, 128).transpose(0, 1, 3, 4, 5, 2, 6)
    m = m.reshape(count, EZ, 3, 2, 8, 128)
    ids = slab_ids.reshape(-1, 128)
    matrices, vectors = constant_tables()
    matrices, vectors = jnp.asarray(matrices), jnp.asarray(vectors)
    hbm = pl.BlockSpec(memory_space=pltpu.HBM)
    vmem = pl.BlockSpec(memory_space=pltpu.VMEM)
    smem = pl.BlockSpec(memory_space=pltpu.SMEM)
    whole = (count, EZ, 2, 8, 128)
    face, z_face, edge = (count, 8, 128), (count // 2, 8, 128), (steps // 2, 8, 128)
    dma = pltpu.SemaphoreType.DMA
    shared = pl.pallas_call(
        main_kernel,
        in_specs=[hbm] * 6,
        out_specs=[vmem] * 7 + [smem],
        out_shape=[pltpu.VMEM(s, F32) for s in (whole, face, face, z_face, edge, edge)]
        + [pltpu.VMEM((count, 128), jnp.int32), pltpu.SMEM((8, 128), jnp.int32)],
        scratch_shapes=[
            pltpu.VMEM(u.shape, F32),
            pltpu.VMEM(m.shape, F32),
            pltpu.VMEM((CHUNK * EZ * 16, 256), BF16),
            pltpu.VMEM((CHUNK * EZ * 16, 256), BF16),
            pltpu.VMEM((CHUNK * EZ * 2, 8, 128), F32),
            pltpu.VMEM((CHUNK, 8, 8, 128), F32),
            pltpu.VMEM(matrices.shape, BF16),
            pltpu.VMEM(vectors.shape, F32),
            pltpu.VMEM(ids.shape, jnp.int32),
            pltpu.VMEM((8, 128), jnp.int32),
            pltpu.VMEM(face, F32),
            pltpu.VMEM(face, F32),
            pltpu.VMEM(z_face, F32),
            pltpu.VMEM(edge, F32),
            pltpu.VMEM(edge, F32),
            dma((2, steps)),
            dma((5,)),
            dma((5,)),
            dma((5,)),
        ],
        compiler_params=pltpu.CompilerParams(
            collective_id=0, has_side_effects=True, vmem_limit_bytes=60 * 2**20
        ),
    )(u, m, matrices, vectors, face_map, ids)
    out = pl.pallas_call(
        final_kernel,
        in_specs=[vmem] * 7 + [smem],
        out_specs=hbm,
        out_shape=jax.ShapeDtypeStruct(whole, F32),
        scratch_shapes=[pltpu.VMEM(whole, F32), pltpu.VMEM((count, 2, 8, 128), F32), dma((count // LAST,))],
        compiler_params=pltpu.CompilerParams(vmem_limit_bytes=40 * 2**20),
    )(*shared)
    out = out.reshape(count, EZ, 2, 2, EY, 128).transpose(0, 1, 4, 2, 3, 5)
    return out.reshape(1, count, EZ, EY, PTS)


def solution(mesh):
    return jax.shard_map(
        body,
        mesh=mesh,
        in_specs=(
            P("layer", "slab", None, None, None),
            P("layer", "slab", None, None, None, None),
            P(),
            P("slab", None),
        ),
        out_specs=P("layer", "slab", None, None, None),
        check_vma=False,
    )
```

```python
import functools

import jax
import jax.numpy as jnp
import numpy as np
from jax import lax
from jax.experimental import pallas as pl
from jax.experimental.pallas import tpu as pltpu
from jax.sharding import PartitionSpec as P

P_SIZE = 8
PTS = 512
EY = 4
EZ = 4
CHUNK = 8
AHEAD = 4
HOLD = 0
FACES, EDGES, BOTH = (0, 1, 2), (3, 4), (0, 1, 2, 3, 4)
LAST = 16
GATHER = 32
F32 = jnp.float32
BF16 = jnp.bfloat16
MESH = pl.DeviceIdType.MESH


def legendre_pair(gll_nodes, degree):
    lower_poly = gll_nodes * 0.0 + 1.0
    upper_poly = gll_nodes.copy()
    for poly_order in range(2, degree + 1):
        lower_poly, upper_poly = (
            upper_poly,
            ((2 * poly_order - 1) * gll_nodes * upper_poly - (poly_order - 1) * lower_poly)
            / poly_order,
        )
    return (lower_poly, upper_poly)


def gll_tables():
    degree = P_SIZE - 1
    gll_nodes = -np.cos(np.pi * np.arange(P_SIZE) / degree)
    for newton_sweep in range(100):
        lower_poly, upper_poly = legendre_pair(gll_nodes, degree)
        gll_nodes = gll_nodes - (gll_nodes * upper_poly - lower_poly) / ((degree + 1) * upper_poly)
    lower_poly, upper_poly = legendre_pair(gll_nodes, degree)
    quad_weights = 2.0 / (degree * (degree + 1) * upper_poly * upper_poly)
    identity = np.eye(P_SIZE)
    differ = gll_nodes[:, None] - gll_nodes[None, :] + identity
    derivative = upper_poly[:, None] / (upper_poly[None, :] * differ)
    derivative = derivative * (1.0 - identity)
    derivative[0, 0] = -degree * (degree + 1) / 4.0
    derivative[degree, degree] = degree * (degree + 1) / 4.0
    return derivative, quad_weights


def parts(table):
    high = np.asarray(table, np.float32).astype(BF16)
    low = (table - high.astype(np.float64)).astype(np.float32).astype(BF16)
    return high, low


def constant_tables():
    derivative, rho = gll_tables()
    eye = np.eye(P_SIZE)
    pair = np.eye(2)
    x_in = np.kron(pair, np.kron(eye, derivative.T))
    y_in = np.kron(pair, np.kron(derivative.T, eye))
    x_out = np.kron(pair, np.kron(eye, derivative))
    y_out = np.kron(pair, np.kron(derivative, eye))
    lane = np.arange(128)[None, :]
    plane = rho[lane // 8 % 8] * rho[lane % 8]
    high, low = parts(np.concatenate([x_in * plane, y_in * plane], 1))
    matrices = [high, low]
    for table in (x_out, y_out):
        matrices.append(np.concatenate(parts(table), 1))
    sub = np.arange(8)[:, None] // 4
    c_low = 2 * sub + lane // 64
    vectors = []
    for table, weight in ((derivative, rho[c_low] * plane), (derivative.T, 1.0)):
        for sign in (1.0, -1.0):
            for move in (0, 1, 2, 3):
                other = c_low ^ move
                term = weight * (table[c_low, other] + sign * table[c_low, 7 - other]) / 2
                vectors.append(np.roll(term, 4, 0) if move > 1 else term)
    for half in range(2):
        vectors.append(rho[4 * half + c_low] + 0.0 * plane)
    return np.stack(matrices), np.stack(vectors).astype(np.float32)


def turn(value, shift):
    return pltpu.roll(value, shift % 128, axis=value.ndim - 1) if shift % 128 else value


def spin(value, shift):
    return turn(value, shift)


def slide(value, shift):
    return pltpu.roll(value, shift % 8, axis=value.ndim - 2)


def mirror(value):
    return slide(turn(value, 64), 4)


def iotas():
    sub = lax.broadcasted_iota(jnp.int32, (8, 128), 0)
    lane = lax.broadcasted_iota(jnp.int32, (8, 128), 1)
    return sub, lane


def split(value):
    high = value.astype(BF16)
    low = (value - high.astype(F32)).astype(BF16)
    return jnp.concatenate([high, low], axis=-1)


def product(both, matrix):
    return jnp.dot(both, jnp.concatenate([matrix, matrix], 0), preferred_element_type=F32)


def along_z(low, high, low_turned, high_turned, table_ref, start):
    back, back_turned = slide(high_turned, 4), slide(high, 4)
    halves = []
    for value, turned, first in (
        (low + back, low_turned + back_turned, start),
        (low - back, low_turned - back_turned, start + 4),
    ):
        near = table_ref[first] * value + table_ref[first + 1] * turned
        far = table_ref[first + 2] * value + table_ref[first + 3] * turned
        halves.append(near + slide(far, 4))
    even, odd = halves
    return even + odd, mirror(odd - even)


def flip_faces(value, sub, lane, shift):
    value = jnp.take_along_axis(value, sub ^ 3, axis=0)
    return jnp.take_along_axis(value, ((((lane - shift) & 127) ^ 56) + shift) & 127, axis=1)


def edge_mask(sub, lane, slot):
    base = jnp.where(sub < 4, 0, 71)
    return ((lane - base - slot) & 71) == 0


def chunk_fluxes(u_ref, m_ref, mat_ref, vec_ref, fx_ref, fy_ref, fz_ref):
    count = u_ref.shape[0]
    rows = count * EZ * 2 * 8
    u = u_ref[...].reshape(rows, 128)
    scaled = u.reshape(count * EZ, 2, 8, 128) * vec_ref[16:18]
    both = split(scaled.reshape(rows, 128))
    grads = product(both, mat_ref[0]) + product(both, mat_ref[1])
    turned = turn(u, 64)
    flux_x, flux_y = [], []
    for s in range(count):
        for ez in range(EZ):
            at = (s * EZ + ez) * 16
            pieces = along_z(
                u[at : at + 8], u[at + 8 : at + 16], turned[at : at + 8], turned[at + 8 : at + 16], vec_ref, 0
            )
            for h in range(2):
                grad = grads[at + 8 * h : at + 8 * h + 8]
                fz_ref[at // 8 + h] = pieces[h] * m_ref[s, ez, 2, h]
                flux_x.append(grad[:, :128] * m_ref[s, ez, 0, h])
                flux_y.append(grad[:, 128:] * m_ref[s, ez, 1, h])
    fx_ref[...] = split(jnp.concatenate(flux_x, 0))
    fy_ref[...] = split(jnp.concatenate(flux_y, 0))


def corners(sub, lane):
    return (sub < 4) & (lane < 64), (sub >= 4) & (lane >= 64)


def chunk_local(fx_ref, fy_ref, fz_ref, mat_ref, vec_ref, sub, lane, put):
    count = CHUNK
    result = product(fx_ref[...], mat_ref[2]) + product(fy_ref[...], mat_ref[3])
    flux_z = [fz_ref[k] for k in range(2 * count * EZ)]
    flux_turned = [turn(value, 64) for value in flux_z]
    out_z = [
        along_z(flux_z[k], flux_z[k + 1], flux_turned[k], flux_turned[k + 1], vec_ref, 8)
        for k in range(0, 2 * count * EZ, 2)
    ]
    b = (lane >> 3) & 7
    ey = sub & 3
    swap = jnp.where((b == 0) | (b == 7), lane ^ 56, lane)
    high_b = (b == 7) & (ey < 3)
    low_b = (b == 0) & (ey > 0)
    bottom, top = corners(sub, lane)
    for s in range(count):
        block = []
        for ez in range(EZ):
            for h in range(2):
                at = (s * EZ + ez) * 16 + 8 * h
                v = result[at : at + 8, :128] + result[at : at + 8, 128:] + out_z[s * EZ + ez][h]
                swapped = jnp.take_along_axis(v, swap, axis=1)
                met = jnp.where(high_b, slide(swapped, -1), jnp.where(low_b, slide(swapped, 1), 0.0))
                block.append(v + met)
        for ez in range(EZ - 1):
            upper, lower = block[2 * ez + 1], block[2 * ez + 2]
            block[2 * ez + 2] = jnp.where(bottom, lower + mirror(upper), lower)
            block[2 * ez + 1] = jnp.where(top, upper + mirror(lower), upper)
        for j in range(8):
            put(s, j, block[j])


def chunk_pack(stage_ref, flip_mask, sub, lane, offset):
    count = CHUNK
    a = lane & 7
    bottom, top = corners(sub, lane)
    lefts, rights, z_own = [], [], []
    for s in range(count):
        left = right = stage_ref[s, 0]
        for j in range(1, 8):
            moved = turn(stage_ref[s, j], j)
            left = jnp.where(a == j, moved, left)
            right = jnp.where(a == j - 1, moved, right)
        right = jnp.where(flip_mask(s), flip_faces(right, sub, lane, 7), right)
        lefts.append(left)
        rights.append(right)
        z_own.append(jnp.where(bottom, stage_ref[s, 0], stage_ref[s, 7]))
    z_pairs = [
        jnp.where(bottom | top, z_own[s], turn(z_own[s + 1], 64)) for s in range(0, count, 2)
    ]
    edges = []
    for faces, shift in ((lefts, 0), (rights, 7)):
        packed = faces[0]
        for s in range(1, count):
            packed = jnp.where(edge_mask(sub, lane, s + shift), turn(faces[s], s), packed)
        moved = slide(packed, 4)
        edges.append(jnp.where(sub < 4, spin(moved, offset - 71 - shift), spin(moved, offset + 71 - shift)))
    return lefts, rights, z_pairs, edges


def positions(wanted, values, offset, count):
    t = lax.broadcasted_iota(jnp.int32, (count, 128), 0)
    lane = lax.broadcasted_iota(jnp.int32, (count, 128), 1)
    column = jnp.sum(jnp.where(lane == t + offset, values, 0).astype(F32), axis=1, keepdims=True)
    hit = column == wanted.astype(F32)
    return jnp.sum(jnp.where(hit, t, 0).astype(F32), axis=0, keepdims=True).astype(jnp.int32)


def main_kernel(
    u_hbm, m_hbm, mat_hbm, vec_hbm, fm_hbm, ids_hbm,
    local, left_in, right_in, z_in, el_in, er_in, fm, pos,
    u_v, m_v, fx, fy, fz, stage, mat, vec, ids, pos_v, left, right, z, el, er,
    in_sem, one_sem, send_sem, recv_sem,
):
    cycle = lax.axis_size("slab")
    me = lax.axis_index("slab")
    layer = lax.axis_index("layer")
    after, before = lax.rem(me + 1, cycle), lax.rem(me + cycle - 1, cycle)
    other = 1 - layer
    peers = [(after, layer), (before, layer), (me, other), (after, other), (before, other)]
    count = local.shape[0]
    steps = count // CHUNK
    total = cycle * count
    barrier = pltpu.get_barrier_semaphore()
    def loads(i):
        part = pl.ds(i * CHUNK, CHUNK)
        return [
            pltpu.make_async_copy(u_hbm.at[part], u_v.at[part], in_sem.at[0, lax.rem(i, AHEAD)]),
            pltpu.make_async_copy(m_hbm.at[part], m_v.at[part], in_sem.at[1, lax.rem(i, AHEAD)]),
        ]

    def once():
        pairs = [(mat_hbm, mat), (vec_hbm, vec), (fm_hbm.at[:, pl.ds(0, 128)], fm), (ids_hbm, ids)]
        return [pltpu.make_async_copy(a, b, one_sem.at[k]) for k, (a, b) in enumerate(pairs)]

    for copy in loads(0) + once():
        copy.start()
    for i in range(1, AHEAD - 1):
        for copy in loads(i):
            copy.start()
    for s, l in peers:
        pl.semaphore_signal(barrier, inc=1, device_id={"slab": s, "layer": l}, device_id_type=MESH)
    for copy in once():
        copy.wait()

    per_row = 128 // count
    rows = [ids[pl.ds(d // per_row, 1), :] for d in (me, before, after)]
    sub, lane = iotas()
    found = []
    for row, device, move in ((rows[1], before, total - 1), (rows[2], after, 1)):
        wanted = rows[0] + move
        wanted = jnp.where(wanted >= total, wanted - total, wanted)
        found.append(positions(wanted, row, lax.rem(device, per_row) * count, count))
    pos_v[...] = jnp.where(sub == 0, found[0], found[1])
    pos_copy = pltpu.make_async_copy(pos_v, pos, one_sem.at[4])
    pos_copy.start()

    def sends(i, chunks, kinds):
        part = pl.ds(i * CHUNK, chunks * CHUNK)
        half = pl.ds(i * (CHUNK // 2), chunks * (CHUNK // 2))
        single = pl.ds(i // 2, chunks // 2)
        jobs = [(right, right_in, part), (left, left_in, part), (z, z_in, half), (er, er_in, single), (el, el_in, single)]
        return [
            pltpu.make_async_remote_copy(
                src_ref=src.at[at],
                dst_ref=dst.at[at],
                send_sem=send_sem.at[k],
                recv_sem=recv_sem.at[k],
                device_id={"slab": s, "layer": l},
                device_id_type=MESH,
            )
            for k, ((src, dst, at), (s, l)) in enumerate(zip(jobs, peers))
            if k in kinds
        ]

    def fluxes(i):
        part = pl.ds(i * CHUNK, CHUNK)
        chunk_fluxes(u_v.at[part], m_v.at[part], mat, vec, fx, fy, fz)

    def assemble(i):
        def put(s, j, value):
            local[i * CHUNK + s, j // 2, j % 2] = value
            stage[s, j] = value

        chunk_local(fx, fy, fz, mat, vec, sub, lane, put)

    def pack(i, odd):
        def flip_mask(s):
            return fm[pl.ds(i * CHUNK + s, 1), :] != lane

        lefts, rights, z_pairs, edges = chunk_pack(stage, flip_mask, sub, lane, 64 * odd)
        for s in range(CHUNK):
            left[i * CHUNK + s] = lefts[s]
            right[i * CHUNK + s] = rights[s]
        for s in range(CHUNK // 2):
            z[i * (CHUNK // 2) + s] = z_pairs[s]
        first_of_two = jnp.where(sub < 4, lane, (lane - 71) & 127) < 64
        for ref, edge in ((el, edges[0]), (er, edges[1])):
            ref[i // 2] = jnp.where(first_of_two, ref[i // 2], edge) if odd else edge

    def arrive(i):
        for copy in loads(i):
            copy.wait()

        @pl.when(i + AHEAD - 1 < steps)
        def _():
            for copy in loads(i + AHEAD - 1):
                copy.start()

    def launch(k):
        @pl.when(k == HOLD)
        def _():
            pl.semaphore_wait(barrier, 5)
            for copy in sends(0, 2 * (HOLD + 1), BOTH):
                copy.start()

        @pl.when(k > HOLD)
        def _():
            for copy in sends(2 * k, 2, BOTH):
                copy.start()

    arrive(0)
    fluxes(0)
    arrive(1)
    assemble(0)
    fluxes(1)

    def step(k, carry):
        arrive(2 * k)
        arrive(2 * k + 1)
        for odd in (0, 1):
            i = 2 * k + odd
            pack(i - 2, odd)
            assemble(i - 1)
            fluxes(i)
        launch(k - 1)
        return carry

    lax.fori_loop(1, steps // 2, step, 0)
    pack(steps - 2, 0)
    assemble(steps - 1)
    for copy in sends(steps - 2, 1, FACES):
        copy.start()
    pack(steps - 1, 1)
    for copy in sends(steps - 1, 1, FACES) + sends(steps - 2, 2, EDGES):
        copy.start()
    pos_copy.wait()
    for copy in sends(0, steps, BOTH):
        copy.wait()


def final_kernel(local, left_in, right_in, z_in, el_in, er_in, fm, pos, out_hbm, out, faces, sem):
    sub, lane = iotas()
    count = local.shape[0]
    per_row = 128 // count
    first = lax.rem(lax.axis_index("slab"), per_row) * count
    on_edge = edge_mask(sub, lane, 0)
    even = (lane & 1) == 0
    a = lane & 7
    on_face = (a == 0) | (a == 7)
    bottom = (sub < 4) & (lane < 64)
    top = (sub >= 4) & (lane >= 64)

    def write(i):
        part = pl.ds(i * LAST, LAST)
        return pltpu.make_async_copy(out.at[part], out_hbm.at[part], sem.at[i])

    def edge(edge_ref, at):
        slot = ((at & 8) << 3) | (at & 7)
        return jnp.where(on_edge, pltpu.roll(edge_ref[at >> 4], (128 - slot) & 127, axis=1), 0.0)

    def gather(i, carry):
        for s in range(GATHER):
            slab = i * GATHER + s
            back, ahead = pos[0, first + slab], pos[1, first + slab]
            low = turn(right_in[back], -7) + edge(er_in, back)
            high = left_in[ahead] + edge(el_in, ahead)
            flipped = fm[pl.ds(slab, 1), :] != lane
            high = turn(jnp.where(flipped, flip_faces(high, sub, lane, 0), high), 7)
            faces[slab, 0] = jnp.where(even, low, high)
            faces[slab, 1] = jnp.where(even, high, low)
        return carry

    lax.fori_loop(0, count // GATHER, gather, 0)

    def step(i, carry):
        for s in range(LAST):
            slab = i * LAST + s
            z = slide(z_in[i * (LAST // 2) + s // 2], 4)
            z = z if s % 2 else turn(z, 64)
            for j in range(8):
                v = local[slab, j // 2, j % 2] + jnp.where(on_face, turn(faces[slab, j % 2], -j), 0.0)
                if j == 0:
                    v += jnp.where(bottom, z, 0.0)
                if j == 7:
                    v += jnp.where(top, z, 0.0)
                out[slab, j // 2, j % 2] = v
        write(i).start()
        return carry

    lax.fori_loop(0, count // LAST, step, 0)

    def finish(i, carry):
        write(i).wait()
        return carry

    lax.fori_loop(0, count // LAST, finish, 0)


def body(nodal_field, metric, slab_ids, face_map):
    count = nodal_field.shape[1]
    steps = count // CHUNK
    u = nodal_field.reshape(count, EZ, EY, 2, 2, 128).transpose(0, 1, 3, 4, 2, 5)
    u = u.reshape(count, EZ, 2, 8, 128)
    m = metric.reshape(count, EZ, EY, 3, 2, 2, 128).transpose(0, 1, 3, 4, 5, 2, 6)
    m = m.reshape(count, EZ, 3, 2, 8, 128)
    ids = slab_ids.reshape(-1, 128)
    matrices, vectors = constant_tables()
    matrices, vectors = jnp.asarray(matrices), jnp.asarray(vectors)
    hbm = pl.BlockSpec(memory_space=pltpu.HBM)
    vmem = pl.BlockSpec(memory_space=pltpu.VMEM)
    smem = pl.BlockSpec(memory_space=pltpu.SMEM)
    whole = (count, EZ, 2, 8, 128)
    face, z_face, edge = (count, 8, 128), (count // 2, 8, 128), (steps // 2, 8, 128)
    dma = pltpu.SemaphoreType.DMA
    shared = pl.pallas_call(
        main_kernel,
        in_specs=[hbm] * 6,
        out_specs=[vmem] * 7 + [smem],
        out_shape=[pltpu.VMEM(s, F32) for s in (whole, face, face, z_face, edge, edge)]
        + [pltpu.VMEM((count, 128), jnp.int32), pltpu.SMEM((8, 128), jnp.int32)],
        scratch_shapes=[
            pltpu.VMEM(u.shape, F32),
            pltpu.VMEM(m.shape, F32),
            pltpu.VMEM((CHUNK * EZ * 16, 256), BF16),
            pltpu.VMEM((CHUNK * EZ * 16, 256), BF16),
            pltpu.VMEM((CHUNK * EZ * 2, 8, 128), F32),
            pltpu.VMEM((CHUNK, 8, 8, 128), F32),
            pltpu.VMEM(matrices.shape, BF16),
            pltpu.VMEM(vectors.shape, F32),
            pltpu.VMEM(ids.shape, jnp.int32),
            pltpu.VMEM((8, 128), jnp.int32),
            pltpu.VMEM(face, F32),
            pltpu.VMEM(face, F32),
            pltpu.VMEM(z_face, F32),
            pltpu.VMEM(edge, F32),
            pltpu.VMEM(edge, F32),
            dma((2, AHEAD)),
            dma((5,)),
            dma((5,)),
            dma((5,)),
        ],
        compiler_params=pltpu.CompilerParams(
            collective_id=0, has_side_effects=True, vmem_limit_bytes=60 * 2**20
        ),
    )(u, m, matrices, vectors, face_map, ids)
    out = pl.pallas_call(
        final_kernel,
        in_specs=[vmem] * 7 + [smem],
        out_specs=hbm,
        out_shape=jax.ShapeDtypeStruct(whole, F32),
        scratch_shapes=[pltpu.VMEM(whole, F32), pltpu.VMEM((count, 2, 8, 128), F32), dma((count // LAST,))],
        compiler_params=pltpu.CompilerParams(vmem_limit_bytes=40 * 2**20),
    )(*shared)
    out = out.reshape(count, EZ, 2, 2, EY, 128).transpose(0, 1, 4, 2, 3, 5)
    return out.reshape(1, count, EZ, EY, PTS)


def solution(mesh):
    return jax.shard_map(
        body,
        mesh=mesh,
        in_specs=(
            P("layer", "slab", None, None, None),
            P("layer", "slab", None, None, None, None),
            P(),
            P("slab", None),
        ),
        out_specs=P("layer", "slab", None, None, None),
        check_vma=False,
    )
```

```python
import functools

import jax
import jax.numpy as jnp
import numpy as np
from jax import lax
from jax.experimental import pallas as pl
from jax.experimental.pallas import tpu as pltpu
from jax.sharding import PartitionSpec as P

P_SIZE = 8
PTS = 512
EY = 4
EZ = 4
CHUNK = 8
AHEAD = 4
HOLD = 0
FACES, EDGES, BOTH = (0, 1, 2), (3, 4), (0, 1, 2, 3, 4)
LAST = 16
GATHER = 32
F32 = jnp.float32
BF16 = jnp.bfloat16
MESH = pl.DeviceIdType.MESH


def legendre_pair(gll_nodes, degree):
    lower_poly = gll_nodes * 0.0 + 1.0
    upper_poly = gll_nodes.copy()
    for poly_order in range(2, degree + 1):
        lower_poly, upper_poly = (
            upper_poly,
            ((2 * poly_order - 1) * gll_nodes * upper_poly - (poly_order - 1) * lower_poly)
            / poly_order,
        )
    return (lower_poly, upper_poly)


def gll_tables():
    degree = P_SIZE - 1
    gll_nodes = -np.cos(np.pi * np.arange(P_SIZE) / degree)
    for newton_sweep in range(100):
        lower_poly, upper_poly = legendre_pair(gll_nodes, degree)
        gll_nodes = gll_nodes - (gll_nodes * upper_poly - lower_poly) / ((degree + 1) * upper_poly)
    lower_poly, upper_poly = legendre_pair(gll_nodes, degree)
    quad_weights = 2.0 / (degree * (degree + 1) * upper_poly * upper_poly)
    identity = np.eye(P_SIZE)
    differ = gll_nodes[:, None] - gll_nodes[None, :] + identity
    derivative = upper_poly[:, None] / (upper_poly[None, :] * differ)
    derivative = derivative * (1.0 - identity)
    derivative[0, 0] = -degree * (degree + 1) / 4.0
    derivative[degree, degree] = degree * (degree + 1) / 4.0
    return derivative, quad_weights


def parts(table):
    high = np.asarray(table, np.float32).astype(BF16)
    low = (table - high.astype(np.float64)).astype(np.float32).astype(BF16)
    return high, low


def constant_tables():
    derivative, rho = gll_tables()
    eye = np.eye(P_SIZE)
    pair = np.eye(2)
    x_in = np.kron(pair, np.kron(eye, derivative.T))
    y_in = np.kron(pair, np.kron(derivative.T, eye))
    x_out = np.kron(pair, np.kron(eye, derivative))
    y_out = np.kron(pair, np.kron(derivative, eye))
    lane = np.arange(128)[None, :]
    plane = rho[lane // 8 % 8] * rho[lane % 8]
    high, low = parts(np.concatenate([x_in * plane, y_in * plane], 1))
    matrices = [high, low]
    for table in (x_out, y_out):
        matrices.append(np.concatenate(parts(table), 1))
    sub = np.arange(8)[:, None] // 4
    c_low = 2 * sub + lane // 64
    vectors = []
    for table, weight in ((derivative, rho[c_low] * plane), (derivative.T, 1.0)):
        for sign in (1.0, -1.0):
            for move in (0, 1, 2, 3):
                other = c_low ^ move
                term = weight * (table[c_low, other] + sign * table[c_low, 7 - other]) / 2
                vectors.append(np.roll(term, 4, 0) if move > 1 else term)
    for half in range(2):
        vectors.append(rho[4 * half + c_low] + 0.0 * plane)
    return np.stack(matrices), np.stack(vectors).astype(np.float32)


def turn(value, shift):
    return pltpu.roll(value, shift % 128, axis=value.ndim - 1) if shift % 128 else value


def spin(value, shift):
    return turn(value, shift)


def slide(value, shift):
    return pltpu.roll(value, shift % 8, axis=value.ndim - 2)


def mirror(value):
    return slide(turn(value, 64), 4)


def iotas():
    sub = lax.broadcasted_iota(jnp.int32, (8, 128), 0)
    lane = lax.broadcasted_iota(jnp.int32, (8, 128), 1)
    return sub, lane


def split(value):
    high = value.astype(BF16)
    low = (value - high.astype(F32)).astype(BF16)
    return jnp.concatenate([high, low], axis=-1)


def product(both, matrix):
    return jnp.dot(both, jnp.concatenate([matrix, matrix], 0), preferred_element_type=F32)


def along_z(low, high, low_turned, high_turned, table_ref, start):
    back, back_turned = slide(high_turned, 4), slide(high, 4)
    halves = []
    for value, turned, first in (
        (low + back, low_turned + back_turned, start),
        (low - back, low_turned - back_turned, start + 4),
    ):
        near = table_ref[first] * value + table_ref[first + 1] * turned
        far = table_ref[first + 2] * value + table_ref[first + 3] * turned
        halves.append(near + slide(far, 4))
    even, odd = halves
    return even + odd, mirror(odd - even)


def flip_faces(value, sub, lane, shift):
    value = jnp.take_along_axis(value, sub ^ 3, axis=0)
    return jnp.take_along_axis(value, ((((lane - shift) & 127) ^ 56) + shift) & 127, axis=1)


def edge_mask(sub, lane, slot):
    base = jnp.where(sub < 4, 0, 71)
    return ((lane - base - slot) & 71) == 0


def chunk_fluxes(u_ref, m_ref, mat_ref, vec_ref, fx_ref, fy_ref, fz_ref):
    count = u_ref.shape[0]
    rows = count * EZ * 2 * 8
    u = u_ref[...].reshape(rows, 128)
    scaled = u.reshape(count * EZ, 2, 8, 128) * vec_ref[16:18]
    both = split(scaled.reshape(rows, 128))
    grads = product(both, mat_ref[0]) + product(both, mat_ref[1])
    turned = turn(u, 64)
    flux_x, flux_y = [], []
    for s in range(count):
        for ez in range(EZ):
            at = (s * EZ + ez) * 16
            pieces = along_z(
                u[at : at + 8], u[at + 8 : at + 16], turned[at : at + 8], turned[at + 8 : at + 16], vec_ref, 0
            )
            for h in range(2):
                grad = grads[at + 8 * h : at + 8 * h + 8]
                fz_ref[at // 8 + h] = pieces[h] * m_ref[s, ez, 2, h]
                flux_x.append(grad[:, :128] * m_ref[s, ez, 0, h])
                flux_y.append(grad[:, 128:] * m_ref[s, ez, 1, h])
    fx_ref[...] = split(jnp.concatenate(flux_x, 0))
    fy_ref[...] = split(jnp.concatenate(flux_y, 0))


def corners(sub, lane):
    return (sub < 4) & (lane < 64), (sub >= 4) & (lane >= 64)


def chunk_local(fx_ref, fy_ref, fz_ref, mat_ref, vec_ref, sub, lane, put):
    count = CHUNK
    result = product(fx_ref[...], mat_ref[2]) + product(fy_ref[...], mat_ref[3])
    flux_z = [fz_ref[k] for k in range(2 * count * EZ)]
    flux_turned = [turn(value, 64) for value in flux_z]
    out_z = [
        along_z(flux_z[k], flux_z[k + 1], flux_turned[k], flux_turned[k + 1], vec_ref, 8)
        for k in range(0, 2 * count * EZ, 2)
    ]
    b = (lane >> 3) & 7
    ey = sub & 3
    swap = jnp.where((b == 0) | (b == 7), lane ^ 56, lane)
    high_b = (b == 7) & (ey < 3)
    low_b = (b == 0) & (ey > 0)
    source = jnp.where(high_b, sub + 1, jnp.where(low_b, sub - 1, sub))
    bottom, top = corners(sub, lane)
    for s in range(count):
        block = []
        for ez in range(EZ):
            for h in range(2):
                at = (s * EZ + ez) * 16 + 8 * h
                v = result[at : at + 8, :128] + result[at : at + 8, 128:] + out_z[s * EZ + ez][h]
                swapped = jnp.take_along_axis(v, swap, axis=1)
                met = jnp.take_along_axis(swapped, source, axis=0)
                block.append(v + jnp.where(high_b | low_b, met, 0.0))
        for ez in range(EZ - 1):
            upper, lower = block[2 * ez + 1], block[2 * ez + 2]
            block[2 * ez + 2] = jnp.where(bottom, lower + mirror(upper), lower)
            block[2 * ez + 1] = jnp.where(top, upper + mirror(lower), upper)
        for j in range(8):
            put(s, j, block[j])


def chunk_pack(stage_ref, flip_mask, sub, lane, offset):
    count = CHUNK
    a = lane & 7
    bottom, top = corners(sub, lane)
    lefts, rights, z_own = [], [], []
    for s in range(count):
        left = right = stage_ref[s, 0]
        for j in range(1, 8):
            moved = turn(stage_ref[s, j], j)
            left = jnp.where(a == j, moved, left)
            right = jnp.where(a == j - 1, moved, right)
        right = jnp.where(flip_mask(s), flip_faces(right, sub, lane, 7), right)
        lefts.append(left)
        rights.append(right)
        z_own.append(jnp.where(bottom, stage_ref[s, 0], stage_ref[s, 7]))
    z_pairs = [
        jnp.where(bottom | top, z_own[s], turn(z_own[s + 1], 64)) for s in range(0, count, 2)
    ]
    edges = []
    for faces, shift in ((lefts, 0), (rights, 7)):
        packed = faces[0]
        for s in range(1, count):
            packed = jnp.where(edge_mask(sub, lane, s + shift), turn(faces[s], s), packed)
        moved = slide(packed, 4)
        edges.append(jnp.where(sub < 4, spin(moved, offset - 71 - shift), spin(moved, offset + 71 - shift)))
    return lefts, rights, z_pairs, edges


def positions(wanted, values, offset, count):
    t = lax.broadcasted_iota(jnp.int32, (count, 128), 0)
    lane = lax.broadcasted_iota(jnp.int32, (count, 128), 1)
    column = jnp.sum(jnp.where(lane == t + offset, values, 0).astype(F32), axis=1, keepdims=True)
    hit = column == wanted.astype(F32)
    return jnp.sum(jnp.where(hit, t, 0).astype(F32), axis=0, keepdims=True).astype(jnp.int32)


def main_kernel(
    u_hbm, m_hbm, mat_hbm, vec_hbm, fm_hbm, ids_hbm,
    local, right_in, er_in, pos,
    left_in, z_in, el_in, fm, u_v, m_v, fx, fy, fz, stage, highs, mat, vec, ids, pos_v, left, right, z, el, er,
    in_sem, one_sem, send_sem, recv_sem,
):
    cycle = lax.axis_size("slab")
    me = lax.axis_index("slab")
    layer = lax.axis_index("layer")
    after, before = lax.rem(me + 1, cycle), lax.rem(me + cycle - 1, cycle)
    other = 1 - layer
    peers = [(after, layer), (before, layer), (me, other), (after, other), (before, other)]
    count = local.shape[0]
    steps = count // CHUNK
    total = cycle * count
    barrier = pltpu.get_barrier_semaphore()
    def loads(i):
        part = pl.ds(i * CHUNK, CHUNK)
        return [
            pltpu.make_async_copy(u_hbm.at[part], u_v.at[part], in_sem.at[0, lax.rem(i, AHEAD)]),
            pltpu.make_async_copy(m_hbm.at[part], m_v.at[part], in_sem.at[1, lax.rem(i, AHEAD)]),
        ]

    def once():
        pairs = [(mat_hbm, mat), (vec_hbm, vec), (fm_hbm.at[:, pl.ds(0, 128)], fm), (ids_hbm, ids)]
        return [pltpu.make_async_copy(a, b, one_sem.at[k]) for k, (a, b) in enumerate(pairs)]

    for copy in loads(0) + once():
        copy.start()
    for i in range(1, AHEAD - 1):
        for copy in loads(i):
            copy.start()
    for s, l in peers:
        pl.semaphore_signal(barrier, inc=1, device_id={"slab": s, "layer": l}, device_id_type=MESH)
    for copy in once()[:2]:
        copy.wait()

    sub, lane = iotas()
    per_row = 128 // count

    def sends(i, chunks, kinds):
        part = pl.ds(i * CHUNK, chunks * CHUNK)
        half = pl.ds(i * (CHUNK // 2), chunks * (CHUNK // 2))
        single = pl.ds(i // 2, chunks // 2)
        jobs = [(right, right_in, part), (left, left_in, part), (z, z_in, half), (er, er_in, single), (el, el_in, single)]
        return [
            pltpu.make_async_remote_copy(
                src_ref=src.at[at],
                dst_ref=dst.at[at],
                send_sem=send_sem.at[k],
                recv_sem=recv_sem.at[k],
                device_id={"slab": s, "layer": l},
                device_id_type=MESH,
            )
            for k, ((src, dst, at), (s, l)) in enumerate(zip(jobs, peers))
            if k in kinds
        ]

    def fluxes(i):
        part = pl.ds(i * CHUNK, CHUNK)
        chunk_fluxes(u_v.at[part], m_v.at[part], mat, vec, fx, fy, fz)

    def assemble(i):
        def put(s, j, value):
            local[i * CHUNK + s, j // 2, j % 2] = value
            stage[s, j] = value

        chunk_local(fx, fy, fz, mat, vec, sub, lane, put)

    def pack(i, odd):
        def flip_mask(s):
            return fm[pl.ds(i * CHUNK + s, 1), :] != lane

        lefts, rights, z_pairs, edges = chunk_pack(stage, flip_mask, sub, lane, 64 * odd)
        for s in range(CHUNK):
            left[i * CHUNK + s] = lefts[s]
            right[i * CHUNK + s] = rights[s]
        for s in range(CHUNK // 2):
            z[i * (CHUNK // 2) + s] = z_pairs[s]
        first_of_two = jnp.where(sub < 4, lane, (lane - 71) & 127) < 64
        for ref, edge in ((el, edges[0]), (er, edges[1])):
            ref[i // 2] = jnp.where(first_of_two, ref[i // 2], edge) if odd else edge

    def arrive(i):
        for copy in loads(i):
            copy.wait()

        @pl.when(i + AHEAD - 1 < steps)
        def _():
            for copy in loads(i + AHEAD - 1):
                copy.start()

    def launch(k):
        @pl.when(k == HOLD)
        def _():
            pl.semaphore_wait(barrier, 5)
            for copy in sends(0, 2 * (HOLD + 1), BOTH):
                copy.start()

        @pl.when(k > HOLD)
        def _():
            for copy in sends(2 * k, 2, BOTH):
                copy.start()

    arrive(0)
    fluxes(0)
    arrive(1)
    for copy in once()[2:]:
        copy.wait()
    rows = [ids[pl.ds(d // per_row, 1), :] for d in (me, before, after)]
    found = []
    for row, device, move in ((rows[1], before, total - 1), (rows[2], after, 1)):
        wanted = rows[0] + move
        wanted = jnp.where(wanted >= total, wanted - total, wanted)
        found.append(positions(wanted, row, lax.rem(device, per_row) * count, count))
    pos_v[...] = jnp.where(sub == 0, found[0], found[1])
    pos_copy = pltpu.make_async_copy(pos_v, pos, one_sem.at[4])
    pos_copy.start()
    assemble(0)
    fluxes(1)

    def step(k, carry):
        arrive(2 * k)
        arrive(2 * k + 1)
        for odd in (0, 1):
            i = 2 * k + odd
            pack(i - 2, odd)
            assemble(i - 1)
            fluxes(i)
        launch(k - 1)
        return carry

    lax.fori_loop(1, steps // 2, step, 0)
    pack(steps - 2, 0)
    assemble(steps - 1)
    for copy in sends(steps - 2, 1, FACES):
        copy.start()
    pack(steps - 1, 1)
    for copy in sends(steps - 1, 1, FACES) + sends(steps - 2, 2, EDGES):
        copy.start()
    pos_copy.wait()
    from_next = sends(0, steps, (1, 2, 4))
    from_back = sends(0, steps, (0, 3))
    for copy in from_next:
        copy.wait_recv()
    first = lax.rem(me, per_row) * count
    on_edge = edge_mask(sub, lane, 0)
    bottom, top = corners(sub, lane)
    on_high = (lane & 7) == 7

    def gather(i, carry):
        for s in range(GATHER):
            slab = i * GATHER + s
            ahead = jnp.clip(pos[1, first + slab], 0, count - 1)
            high = left_in[ahead] + edge_of(el_in, ahead, 0, on_edge)
            flipped = fm[pl.ds(slab, 1), :] != lane
            highs[slab] = jnp.where(flipped, flip_faces(high, sub, lane, 0), high)
        return carry

    lax.fori_loop(0, count // GATHER, gather, 0)

    def add_high(i, carry):
        for s in range(LAST):
            slab = i * LAST + s
            whole = z_in[i * (LAST // 2) + s // 2]
            across = slide(whole, 4)
            across = across if s % 2 else turn(across, 64)
            for j in range(8):
                v = local[slab, j // 2, j % 2] + jnp.where(on_high, turn(highs[slab], 7 - j), 0.0)
                if j == 0:
                    v += jnp.where(bottom, across, 0.0)
                if j == 7:
                    v += jnp.where(top, across, 0.0)
                local[slab, j // 2, j % 2] = v
        return carry

    lax.fori_loop(0, count // LAST, add_high, 0)
    for copy in from_back:
        copy.wait_recv()
    for copy in from_next + from_back:
        copy.wait_send()


def edge_of(edge_ref, at, shift, mask):
    slot = ((at & 8) << 3) | (at & 7)
    return jnp.where(mask, pltpu.roll(edge_ref[at >> 4], (128 + shift - slot) & 127, axis=1), 0.0)


def final_kernel(local, right_in, er_in, pos, out_hbm, out, sem):
    sub, lane = iotas()
    count = local.shape[0]
    per_row = 128 // count
    first = lax.rem(lax.axis_index("slab"), per_row) * count
    on_edge = edge_mask(sub, lane, 7)
    on_low = (lane & 7) == 0

    def write(i):
        part = pl.ds(i * LAST, LAST)
        return pltpu.make_async_copy(out.at[part], out_hbm.at[part], sem.at[i])

    def step(i, carry):
        for s in range(LAST):
            slab = i * LAST + s
            back = jnp.clip(pos[0, first + slab], 0, count - 1)
            low = right_in[back] + edge_of(er_in, back, 7, on_edge)
            for j in range(8):
                v = local[slab, j // 2, j % 2] + jnp.where(on_low, turn(low, -7 - j), 0.0)
                out[slab, j // 2, j % 2] = v
        write(i).start()
        return carry

    lax.fori_loop(0, count // LAST, step, 0)

    def finish(i, carry):
        write(i).wait()
        return carry

    lax.fori_loop(0, count // LAST, finish, 0)


def body(nodal_field, metric, slab_ids, face_map):
    count = nodal_field.shape[1]
    steps = count // CHUNK
    u = nodal_field.reshape(count, EZ, EY, 2, 2, 128).transpose(0, 1, 3, 4, 2, 5)
    u = u.reshape(count, EZ, 2, 8, 128)
    m = metric.reshape(count, EZ, EY, 3, 2, 2, 128).transpose(0, 1, 3, 4, 5, 2, 6)
    m = m.reshape(count, EZ, 3, 2, 8, 128)
    ids = slab_ids.reshape(-1, 128)
    matrices, vectors = constant_tables()
    matrices, vectors = jnp.asarray(matrices), jnp.asarray(vectors)
    hbm = pl.BlockSpec(memory_space=pltpu.HBM)
    vmem = pl.BlockSpec(memory_space=pltpu.VMEM)
    smem = pl.BlockSpec(memory_space=pltpu.SMEM)
    whole = (count, EZ, 2, 8, 128)
    face, z_face, edge = (count, 8, 128), (count // 2, 8, 128), (steps // 2, 8, 128)
    dma = pltpu.SemaphoreType.DMA
    shared = pl.pallas_call(
        main_kernel,
        in_specs=[hbm] * 6,
        out_specs=[vmem] * 3 + [smem],
        out_shape=[pltpu.VMEM(s, F32) for s in (whole, face, edge)] + [pltpu.SMEM((8, 128), jnp.int32)],
        scratch_shapes=[
            pltpu.VMEM(face, F32),
            pltpu.VMEM(z_face, F32),
            pltpu.VMEM(edge, F32),
            pltpu.VMEM((count, 128), jnp.int32),
            pltpu.VMEM(u.shape, F32),
            pltpu.VMEM(m.shape, F32),
            pltpu.VMEM((CHUNK * EZ * 16, 256), BF16),
            pltpu.VMEM((CHUNK * EZ * 16, 256), BF16),
            pltpu.VMEM((CHUNK * EZ * 2, 8, 128), F32),
            pltpu.VMEM((CHUNK, 8, 8, 128), F32),
            pltpu.VMEM(face, F32),
            pltpu.VMEM(matrices.shape, BF16),
            pltpu.VMEM(vectors.shape, F32),
            pltpu.VMEM(ids.shape, jnp.int32),
            pltpu.VMEM((8, 128), jnp.int32),
            pltpu.VMEM(face, F32),
            pltpu.VMEM(face, F32),
            pltpu.VMEM(z_face, F32),
            pltpu.VMEM(edge, F32),
            pltpu.VMEM(edge, F32),
            dma((2, AHEAD)),
            dma((5,)),
            dma((5,)),
            dma((5,)),
        ],
        compiler_params=pltpu.CompilerParams(
            collective_id=0, has_side_effects=True, vmem_limit_bytes=60 * 2**20
        ),
    )(u, m, matrices, vectors, face_map, ids)
    out = pl.pallas_call(
        final_kernel,
        in_specs=[vmem] * 3 + [smem],
        out_specs=hbm,
        out_shape=jax.ShapeDtypeStruct(whole, F32),
        scratch_shapes=[pltpu.VMEM(whole, F32), dma((count // LAST,))],
        compiler_params=pltpu.CompilerParams(vmem_limit_bytes=40 * 2**20),
    )(*shared)
    out = out.reshape(count, EZ, 2, 2, EY, 128).transpose(0, 1, 4, 2, 3, 5)
    return out.reshape(1, count, EZ, EY, PTS)


def solution(mesh):
    return jax.shard_map(
        body,
        mesh=mesh,
        in_specs=(
            P("layer", "slab", None, None, None),
            P("layer", "slab", None, None, None, None),
            P(),
            P("slab", None),
        ),
        out_specs=P("layer", "slab", None, None, None),
        check_vma=False,
    )
```

```python
import functools

import jax
import jax.numpy as jnp
import numpy as np
from jax import lax
from jax.experimental import pallas as pl
from jax.experimental.pallas import tpu as pltpu
from jax.sharding import PartitionSpec as P

P_SIZE = 8
PTS = 512
EY = 4
EZ = 4
CHUNK = 8
AHEAD = 4
HOLD = 0
FACES, EDGES, BOTH = (0, 1, 2), (3, 4), (0, 1, 2, 3, 4)
LAST = 16
GATHER = 32
F32 = jnp.float32
BF16 = jnp.bfloat16
MESH = pl.DeviceIdType.MESH


def legendre_pair(gll_nodes, degree):
    lower_poly = gll_nodes * 0.0 + 1.0
    upper_poly = gll_nodes.copy()
    for poly_order in range(2, degree + 1):
        lower_poly, upper_poly = (
            upper_poly,
            ((2 * poly_order - 1) * gll_nodes * upper_poly - (poly_order - 1) * lower_poly)
            / poly_order,
        )
    return (lower_poly, upper_poly)


def gll_tables():
    degree = P_SIZE - 1
    gll_nodes = -np.cos(np.pi * np.arange(P_SIZE) / degree)
    for newton_sweep in range(100):
        lower_poly, upper_poly = legendre_pair(gll_nodes, degree)
        gll_nodes = gll_nodes - (gll_nodes * upper_poly - lower_poly) / ((degree + 1) * upper_poly)
    lower_poly, upper_poly = legendre_pair(gll_nodes, degree)
    quad_weights = 2.0 / (degree * (degree + 1) * upper_poly * upper_poly)
    identity = np.eye(P_SIZE)
    differ = gll_nodes[:, None] - gll_nodes[None, :] + identity
    derivative = upper_poly[:, None] / (upper_poly[None, :] * differ)
    derivative = derivative * (1.0 - identity)
    derivative[0, 0] = -degree * (degree + 1) / 4.0
    derivative[degree, degree] = degree * (degree + 1) / 4.0
    return derivative, quad_weights


def parts(table):
    high = np.asarray(table, np.float32).astype(BF16)
    low = (table - high.astype(np.float64)).astype(np.float32).astype(BF16)
    return high, low


def constant_tables():
    derivative, rho = gll_tables()
    eye = np.eye(P_SIZE)
    pair = np.eye(2)
    x_in = np.kron(pair, np.kron(eye, derivative.T))
    y_in = np.kron(pair, np.kron(derivative.T, eye))
    x_out = np.kron(pair, np.kron(eye, derivative))
    y_out = np.kron(pair, np.kron(derivative, eye))
    lane = np.arange(128)[None, :]
    plane = rho[lane // 8 % 8] * rho[lane % 8]
    high, low = parts(np.concatenate([x_in * plane, y_in * plane], 1))
    matrices = [high, low]
    for table in (x_out, y_out):
        matrices.append(np.concatenate(parts(table), 1))
    sub = np.arange(8)[:, None] // 4
    c_low = 2 * sub + lane // 64
    vectors = []
    for table, weight in ((derivative, rho[c_low] * plane), (derivative.T, 1.0)):
        for sign in (1.0, -1.0):
            for move in (0, 1, 2, 3):
                other = c_low ^ move
                term = weight * (table[c_low, other] + sign * table[c_low, 7 - other]) / 2
                vectors.append(np.roll(term, 4, 0) if move > 1 else term)
    for half in range(2):
        vectors.append(rho[4 * half + c_low] + 0.0 * plane)
    return np.stack(matrices), np.stack(vectors).astype(np.float32)


def turn(value, shift):
    return pltpu.roll(value, shift % 128, axis=value.ndim - 1) if shift % 128 else value


def spin(value, shift):
    return turn(value, shift)


def slide(value, shift):
    return pltpu.roll(value, shift % 8, axis=value.ndim - 2)


def mirror(value):
    return slide(turn(value, 64), 4)


def iotas():
    sub = lax.broadcasted_iota(jnp.int32, (8, 128), 0)
    lane = lax.broadcasted_iota(jnp.int32, (8, 128), 1)
    return sub, lane


def split(value):
    high = value.astype(BF16)
    low = (value - high.astype(F32)).astype(BF16)
    return jnp.concatenate([high, low], axis=-1)


def product(both, matrix):
    return jnp.dot(both, jnp.concatenate([matrix, matrix], 0), preferred_element_type=F32)


def along_z(low, high, low_turned, high_turned, table_ref, start):
    back, back_turned = slide(high_turned, 4), slide(high, 4)
    halves = []
    for value, turned, first in (
        (low + back, low_turned + back_turned, start),
        (low - back, low_turned - back_turned, start + 4),
    ):
        near = table_ref[first] * value + table_ref[first + 1] * turned
        far = table_ref[first + 2] * value + table_ref[first + 3] * turned
        halves.append(near + slide(far, 4))
    even, odd = halves
    return even + odd, mirror(odd - even)


def flip_faces(value, sub, lane, shift):
    value = jnp.take_along_axis(value, sub ^ 3, axis=0)
    return jnp.take_along_axis(value, ((((lane - shift) & 127) ^ 56) + shift) & 127, axis=1)


def edge_mask(sub, lane, slot):
    base = jnp.where(sub < 4, 0, 71)
    return ((lane - base - slot) & 71) == 0


def chunk_fluxes(u_ref, m_ref, mat_ref, vec_ref, fx_ref, fy_ref, fz_ref):
    count = u_ref.shape[0]
    rows = count * EZ * 2 * 8
    u = u_ref[...].reshape(rows, 128)
    scaled = u.reshape(count * EZ, 2, 8, 128) * vec_ref[16:18]
    both = split(scaled.reshape(rows, 128))
    grads = product(both, mat_ref[0]) + product(both, mat_ref[1])
    turned = turn(u, 64)
    flux_x, flux_y = [], []
    for s in range(count):
        for ez in range(EZ):
            at = (s * EZ + ez) * 16
            pieces = along_z(
                u[at : at + 8], u[at + 8 : at + 16], turned[at : at + 8], turned[at + 8 : at + 16], vec_ref, 0
            )
            for h in range(2):
                grad = grads[at + 8 * h : at + 8 * h + 8]
                fz_ref[at // 8 + h] = pieces[h] * m_ref[s, ez, 2, h]
                flux_x.append(grad[:, :128] * m_ref[s, ez, 0, h])
                flux_y.append(grad[:, 128:] * m_ref[s, ez, 1, h])
    fx_ref[...] = split(jnp.concatenate(flux_x, 0))
    fy_ref[...] = split(jnp.concatenate(flux_y, 0))


def corners(sub, lane):
    return (sub < 4) & (lane < 64), (sub >= 4) & (lane >= 64)


def chunk_local(fx_ref, fy_ref, fz_ref, mat_ref, vec_ref, sub, lane, put):
    count = CHUNK
    result = product(fx_ref[...], mat_ref[2]) + product(fy_ref[...], mat_ref[3])
    flux_z = [fz_ref[k] for k in range(2 * count * EZ)]
    flux_turned = [turn(value, 64) for value in flux_z]
    out_z = [
        along_z(flux_z[k], flux_z[k + 1], flux_turned[k], flux_turned[k + 1], vec_ref, 8)
        for k in range(0, 2 * count * EZ, 2)
    ]
    b = (lane >> 3) & 7
    ey = sub & 3
    swap = jnp.where((b == 0) | (b == 7), lane ^ 56, lane)
    high_b = (b == 7) & (ey < 3)
    low_b = (b == 0) & (ey > 0)
    source = jnp.where(high_b, sub + 1, jnp.where(low_b, sub - 1, sub))
    bottom, top = corners(sub, lane)
    for s in range(count):
        block = []
        for ez in range(EZ):
            for h in range(2):
                at = (s * EZ + ez) * 16 + 8 * h
                v = result[at : at + 8, :128] + result[at : at + 8, 128:] + out_z[s * EZ + ez][h]
                swapped = jnp.take_along_axis(v, swap, axis=1)
                met = jnp.take_along_axis(swapped, source, axis=0)
                block.append(v + jnp.where(high_b | low_b, met, 0.0))
        for ez in range(EZ - 1):
            upper, lower = block[2 * ez + 1], block[2 * ez + 2]
            block[2 * ez + 2] = jnp.where(bottom, lower + mirror(upper), lower)
            block[2 * ez + 1] = jnp.where(top, upper + mirror(lower), upper)
        for j in range(8):
            put(s, j, block[j])


def chunk_pack(stage_ref, flip_mask, sub, lane, offset):
    count = CHUNK
    a = lane & 7
    bottom, top = corners(sub, lane)
    lefts, rights, z_own = [], [], []
    for s in range(count):
        left = right = stage_ref[s, 0]
        for j in range(1, 8):
            moved = turn(stage_ref[s, j], j)
            left = jnp.where(a == j, moved, left)
            right = jnp.where(a == j - 1, moved, right)
        right = jnp.where(flip_mask(s), flip_faces(right, sub, lane, 7), right)
        lefts.append(left)
        rights.append(right)
        z_own.append(jnp.where(bottom, stage_ref[s, 0], stage_ref[s, 7]))
    z_pairs = [
        jnp.where(bottom | top, z_own[s], turn(z_own[s + 1], 64)) for s in range(0, count, 2)
    ]
    edges = []
    for faces, shift in ((lefts, 0), (rights, 7)):
        packed = faces[0]
        for s in range(1, count):
            packed = jnp.where(edge_mask(sub, lane, s + shift), turn(faces[s], s), packed)
        moved = slide(packed, 4)
        edges.append(jnp.where(sub < 4, spin(moved, offset - 71 - shift), spin(moved, offset + 71 - shift)))
    return lefts, rights, z_pairs, edges


def positions(wanted, values, offset, count):
    t = lax.broadcasted_iota(jnp.int32, (count, 128), 0)
    lane = lax.broadcasted_iota(jnp.int32, (count, 128), 1)
    column = jnp.sum(jnp.where(lane == t + offset, values, 0).astype(F32), axis=1, keepdims=True)
    hit = column == wanted.astype(F32)
    return jnp.sum(jnp.where(hit, t, 0).astype(F32), axis=0, keepdims=True).astype(jnp.int32)


def main_kernel(
    u_hbm, m_hbm, mat_hbm, vec_hbm, fm_hbm, ids_hbm,
    local, right_in, er_in, pos,
    left_in, z_in, el_in, fm, u_v, m_v, fx, fy, fz, stage, highs, mat, vec, ids, pos_v, left, right, z, el, er,
    in_sem, one_sem, send_sem, recv_sem,
):
    cycle = lax.axis_size("slab")
    me = lax.axis_index("slab")
    layer = lax.axis_index("layer")
    after, before = lax.rem(me + 1, cycle), lax.rem(me + cycle - 1, cycle)
    other = 1 - layer
    peers = [(after, layer), (before, layer), (me, other), (after, other), (before, other)]
    count = local.shape[0]
    steps = count // CHUNK
    total = cycle * count
    barrier = pltpu.get_barrier_semaphore()
    def loads(i):
        part = pl.ds(i * CHUNK, CHUNK)
        return [
            pltpu.make_async_copy(u_hbm.at[part], u_v.at[part], in_sem.at[0, lax.rem(i, AHEAD)]),
            pltpu.make_async_copy(m_hbm.at[part], m_v.at[part], in_sem.at[1, lax.rem(i, AHEAD)]),
        ]

    def once():
        pairs = [(mat_hbm, mat), (vec_hbm, vec), (fm_hbm.at[:, pl.ds(0, 128)], fm), (ids_hbm, ids)]
        return [pltpu.make_async_copy(a, b, one_sem.at[k]) for k, (a, b) in enumerate(pairs)]

    for copy in loads(0) + once():
        copy.start()
    for i in range(1, AHEAD - 1):
        for copy in loads(i):
            copy.start()
    for s, l in peers:
        pl.semaphore_signal(barrier, inc=1, device_id={"slab": s, "layer": l}, device_id_type=MESH)
    for copy in once()[:2]:
        copy.wait()

    sub, lane = iotas()
    per_row = 128 // count

    def sends(i, chunks, kinds):
        part = pl.ds(i * CHUNK, chunks * CHUNK)
        half = pl.ds(i * (CHUNK // 2), chunks * (CHUNK // 2))
        single = pl.ds(i // 2, chunks // 2)
        jobs = [(right, right_in, part), (left, left_in, part), (z, z_in, half), (er, er_in, single), (el, el_in, single)]
        return [
            pltpu.make_async_remote_copy(
                src_ref=src.at[at],
                dst_ref=dst.at[at],
                send_sem=send_sem.at[k],
                recv_sem=recv_sem.at[k],
                device_id={"slab": s, "layer": l},
                device_id_type=MESH,
            )
            for k, ((src, dst, at), (s, l)) in enumerate(zip(jobs, peers))
            if k in kinds
        ]

    def fluxes(i):
        part = pl.ds(i * CHUNK, CHUNK)
        chunk_fluxes(u_v.at[part], m_v.at[part], mat, vec, fx, fy, fz)

    def assemble(i):
        def put(s, j, value):
            local[i * CHUNK + s, j // 2, j % 2] = value
            stage[s, j] = value

        chunk_local(fx, fy, fz, mat, vec, sub, lane, put)

    def pack(i, odd):
        def flip_mask(s):
            return fm[pl.ds(i * CHUNK + s, 1), :] != lane

        lefts, rights, z_pairs, edges = chunk_pack(stage, flip_mask, sub, lane, 64 * odd)
        for s in range(CHUNK):
            left[i * CHUNK + s] = lefts[s]
            right[i * CHUNK + s] = rights[s]
        for s in range(CHUNK // 2):
            z[i * (CHUNK // 2) + s] = z_pairs[s]
        first_of_two = jnp.where(sub < 4, lane, (lane - 71) & 127) < 64
        for ref, edge in ((el, edges[0]), (er, edges[1])):
            ref[i // 2] = jnp.where(first_of_two, ref[i // 2], edge) if odd else edge

    def arrive(i):
        for copy in loads(i):
            copy.wait()

        @pl.when(i + AHEAD - 1 < steps)
        def _():
            for copy in loads(i + AHEAD - 1):
                copy.start()

    def launch(k):
        @pl.when(k == HOLD)
        def _():
            pl.semaphore_wait(barrier, 5)
            for copy in sends(0, 2 * (HOLD + 1), BOTH):
                copy.start()

        @pl.when(k > HOLD)
        def _():
            for copy in sends(2 * k, 2, BOTH):
                copy.start()

    arrive(0)
    fluxes(0)
    arrive(1)
    for copy in once()[2:]:
        copy.wait()
    rows = [ids[pl.ds(d // per_row, 1), :] for d in (me, before, after)]
    found = []
    for row, device, move in ((rows[1], before, total - 1), (rows[2], after, 1)):
        wanted = rows[0] + move
        wanted = jnp.where(wanted >= total, wanted - total, wanted)
        found.append(positions(wanted, row, lax.rem(device, per_row) * count, count))
    pos_v[...] = jnp.where(sub == 0, found[0], found[1])
    pos_copy = pltpu.make_async_copy(pos_v, pos, one_sem.at[4])
    pos_copy.start()
    assemble(0)
    fluxes(1)

    def step(k, carry):
        arrive(2 * k)
        arrive(2 * k + 1)
        for odd in (0, 1):
            i = 2 * k + odd
            pack(i - 2, odd)
            assemble(i - 1)
            fluxes(i)
        launch(k - 1)
        return carry

    lax.fori_loop(1, steps // 2, step, 0)
    pack(steps - 2, 0)
    assemble(steps - 1)
    for copy in sends(steps - 2, 1, FACES):
        copy.start()
    pack(steps - 1, 1)
    for copy in sends(steps - 1, 1, (0,)) + sends(steps - 2, 2, (3,)) + sends(steps - 1, 1, (1, 2)) + sends(steps - 2, 2, (4,)):
        copy.start()
    pos_copy.wait()
    from_next = sends(0, steps, (1, 2, 4))
    from_back = sends(0, steps, (0, 3))
    for copy in from_next:
        copy.wait_recv()
    first = lax.rem(me, per_row) * count
    on_edge = edge_mask(sub, lane, 0)
    bottom, top = corners(sub, lane)
    on_high = (lane & 7) == 7

    def gather(i, carry):
        for s in range(GATHER):
            slab = i * GATHER + s
            ahead = jnp.clip(pos[1, first + slab], 0, count - 1)
            high = left_in[ahead] + edge_of(el_in, ahead, 0, on_edge)
            flipped = fm[pl.ds(slab, 1), :] != lane
            highs[slab] = jnp.where(flipped, flip_faces(high, sub, lane, 0), high)
        return carry

    lax.fori_loop(0, count // GATHER, gather, 0)

    def add_high(i, carry):
        for s in range(LAST):
            slab = i * LAST + s
            whole = z_in[i * (LAST // 2) + s // 2]
            across = slide(whole, 4)
            across = across if s % 2 else turn(across, 64)
            for j in range(8):
                v = local[slab, j // 2, j % 2] + jnp.where(on_high, turn(highs[slab], 7 - j), 0.0)
                if j == 0:
                    v += jnp.where(bottom, across, 0.0)
                if j == 7:
                    v += jnp.where(top, across, 0.0)
                local[slab, j // 2, j % 2] = v
        return carry

    lax.fori_loop(0, count // LAST, add_high, 0)
    for copy in from_back:
        copy.wait_recv()
    for copy in from_next + from_back:
        copy.wait_send()


def edge_of(edge_ref, at, shift, mask):
    slot = ((at & 8) << 3) | (at & 7)
    return jnp.where(mask, pltpu.roll(edge_ref[at >> 4], (128 + shift - slot) & 127, axis=1), 0.0)


def final_kernel(local, right_in, er_in, pos, out_hbm, out, sem):
    sub, lane = iotas()
    count = local.shape[0]
    per_row = 128 // count
    first = lax.rem(lax.axis_index("slab"), per_row) * count
    on_edge = edge_mask(sub, lane, 7)
    on_low = (lane & 7) == 0

    def write(i):
        part = pl.ds(i * LAST, LAST)
        return pltpu.make_async_copy(out.at[part], out_hbm.at[part], sem.at[i])

    def step(i, carry):
        for s in range(LAST):
            slab = i * LAST + s
            back = jnp.clip(pos[0, first + slab], 0, count - 1)
            low = right_in[back] + edge_of(er_in, back, 7, on_edge)
            for j in range(8):
                v = local[slab, j // 2, j % 2] + jnp.where(on_low, turn(low, -7 - j), 0.0)
                out[slab, j // 2, j % 2] = v
        write(i).start()
        return carry

    lax.fori_loop(0, count // LAST, step, 0)

    def finish(i, carry):
        write(i).wait()
        return carry

    lax.fori_loop(0, count // LAST, finish, 0)


def body(nodal_field, metric, slab_ids, face_map):
    count = nodal_field.shape[1]
    steps = count // CHUNK
    u = nodal_field.reshape(count, EZ, EY, 2, 2, 128).transpose(0, 1, 3, 4, 2, 5)
    u = u.reshape(count, EZ, 2, 8, 128)
    m = metric.reshape(count, EZ, EY, 3, 2, 2, 128).transpose(0, 1, 3, 4, 5, 2, 6)
    m = m.reshape(count, EZ, 3, 2, 8, 128)
    ids = slab_ids.reshape(-1, 128)
    matrices, vectors = constant_tables()
    matrices, vectors = jnp.asarray(matrices), jnp.asarray(vectors)
    hbm = pl.BlockSpec(memory_space=pltpu.HBM)
    vmem = pl.BlockSpec(memory_space=pltpu.VMEM)
    smem = pl.BlockSpec(memory_space=pltpu.SMEM)
    whole = (count, EZ, 2, 8, 128)
    face, z_face, edge = (count, 8, 128), (count // 2, 8, 128), (steps // 2, 8, 128)
    dma = pltpu.SemaphoreType.DMA
    shared = pl.pallas_call(
        main_kernel,
        in_specs=[hbm] * 6,
        out_specs=[vmem] * 3 + [smem],
        out_shape=[pltpu.VMEM(s, F32) for s in (whole, face, edge)] + [pltpu.SMEM((8, 128), jnp.int32)],
        scratch_shapes=[
            pltpu.VMEM(face, F32),
            pltpu.VMEM(z_face, F32),
            pltpu.VMEM(edge, F32),
            pltpu.VMEM((count, 128), jnp.int32),
            pltpu.VMEM(u.shape, F32),
            pltpu.VMEM(m.shape, F32),
            pltpu.VMEM((CHUNK * EZ * 16, 256), BF16),
            pltpu.VMEM((CHUNK * EZ * 16, 256), BF16),
            pltpu.VMEM((CHUNK * EZ * 2, 8, 128), F32),
            pltpu.VMEM((CHUNK, 8, 8, 128), F32),
            pltpu.VMEM(face, F32),
            pltpu.VMEM(matrices.shape, BF16),
            pltpu.VMEM(vectors.shape, F32),
            pltpu.VMEM(ids.shape, jnp.int32),
            pltpu.VMEM((8, 128), jnp.int32),
            pltpu.VMEM(face, F32),
            pltpu.VMEM(face, F32),
            pltpu.VMEM(z_face, F32),
            pltpu.VMEM(edge, F32),
            pltpu.VMEM(edge, F32),
            dma((2, AHEAD)),
            dma((5,)),
            dma((5,)),
            dma((5,)),
        ],
        compiler_params=pltpu.CompilerParams(
            collective_id=0, has_side_effects=True, vmem_limit_bytes=60 * 2**20
        ),
    )(u, m, matrices, vectors, face_map, ids)
    out = pl.pallas_call(
        final_kernel,
        in_specs=[vmem] * 3 + [smem],
        out_specs=hbm,
        out_shape=jax.ShapeDtypeStruct(whole, F32),
        scratch_shapes=[pltpu.VMEM(whole, F32), dma((count // LAST,))],
        compiler_params=pltpu.CompilerParams(vmem_limit_bytes=40 * 2**20),
    )(*shared)
    out = out.reshape(count, EZ, 2, 2, EY, 128).transpose(0, 1, 4, 2, 3, 5)
    return out.reshape(1, count, EZ, EY, PTS)


def solution(mesh):
    return jax.shard_map(
        body,
        mesh=mesh,
        in_specs=(
            P("layer", "slab", None, None, None),
            P("layer", "slab", None, None, None, None),
            P(),
            P("slab", None),
        ),
        out_specs=P("layer", "slab", None, None, None),
        check_vma=False,
    )
```
